32 devices in a mesh: ba: 8 (over z, y), dev: 4 (over x, core).
Axes of the slice: x: 2, y: 2, z: 4, core: 2. Of those that a mesh axis runs over, the one named last changes fastest.
Arguments:
- factors: bfloat16 [16, 512, 1024], P('ba', 'dev'), may hold values from -0.1875 to 0.1875
- amplitudes: bfloat16 [64, 512, 512], P(None, 'dev'), may hold values from -0.375 to 0.375
- pair_order: int32 [64], replicated, may hold values from 0 to 63, each once
- occ_bin: int32 [8], replicated, may hold values from 0 to 127
- vir_bin: int32 [16], replicated, may hold values from 0 to 127
- levels: float32 [128], replicated, may hold values from 0.1 to 0.8
Outputs:
- update: float32 [16, 1024], P('ba', 'dev')
The draws below stay inside these ranges and needn't reach their ends.
Inputs may be any that keep to these rules, and one draw needn't show every extreme that they name: `pair_order`: each value appears once; entry k names the ordered occupied pair (value // 8, value % 8). `occ_bin`: orbital i has energy minus levels at its bin. `vir_bin`: window virtual a has energy levels at its bin.
All inputs are finite; a program needn't handle non-finite values.
Results may differ from the reference program's by a relative error of at most 0.0029.
Values may be sent and summed in bfloat16 or wider, within the bound.
A program may use at most 64 MiB of HBM per device.

```python
import jax
import jax.numpy as jnp
from jax import lax

V = 512
NAUX = 1024
NOCC = 8
LEVELS = 128
NW = 16
P_SIZE = 64


def touch_ends(entries, own_key, low, largest):
    longest = entries.shape.index(max(entries.shape))
    spots = []
    for shift in (0, 1):
        where = [jax.random.randint(jax.random.fold_in(own_key, axis), (), 0, length) for axis, length in enumerate(entries.shape)]
        where[longest] = (where[longest] + shift) % entries.shape[longest]
        spots.append(tuple(where))
    return entries.at[spots[0]].set(low).at[spots[1]].set(largest)


def steps_of(key, dims, pieces, least, largest):
    loudness, own = 1.0, jax.random.fold_in(key, 6)
    for axis_at, blocks in pieces:
        draws = jnp.exp(jax.random.uniform(jax.random.fold_in(own, axis_at), (blocks,), jnp.float32, least / len(pieces), largest / len(pieces)))
        loudness = loudness * jnp.repeat(draws, dims[axis_at] // blocks).reshape([-1 if axis == axis_at else 1 for axis in range(len(dims))])
    return loudness


def bell_draw(rng, shape, deviation, bound, shards=(), kind=jnp.bfloat16):
    factor_of = steps_of(rng, shape, shards, -0.22, 0.18) if shards else 1.0
    array = jax.random.normal(rng, shape, jnp.float32) * deviation * factor_of
    return jnp.minimum(jnp.maximum(array, -bound), bound).astype(kind)


def setup_inputs(seed: int = 0) -> dict:
    splits = jax.random.split(jax.random.key(seed), 7)
    factors = bell_draw(splits[0], (NW, V, NAUX), NAUX ** -0.5, 0.1875, ((0, 8), (1, 4)))
    amplitudes = bell_draw(splits[1], (P_SIZE, V, V), (V * V // NAUX) ** -0.5, 0.375, ((1, 4),))
    pair_order = jax.random.permutation(splits[2], P_SIZE).astype(jnp.int32)
    occ_bin = touch_ends(jax.random.randint(splits[3], (NOCC,), 0, LEVELS), jax.random.fold_in(splits[3], 1), 0, LEVELS - 1).astype(jnp.int32)
    vir_bin = touch_ends(jax.random.randint(splits[4], (NW,), 0, LEVELS), jax.random.fold_in(splits[4], 1), 0, LEVELS - 1).astype(jnp.int32)
    levels = jnp.clip(jax.random.uniform(splits[5], (LEVELS,), jnp.float32, 0.1, 0.8), 0.1, 0.8)
    return {"factors": factors, "amplitudes": amplitudes, "pair_order": pair_order, "occ_bin": occ_bin, "vir_bin": vir_bin, "levels": levels}


level_shift = 0.3


def reference(factors, amplitudes, pair_order, occ_bin, vir_bin, levels):
    flat_rows = factors.reshape(NW * V, NAUX)
    flat_amps = amplitudes.reshape(P_SIZE, V * V)

    def one_column(slab):
        integrals = lax.dot_general(flat_rows, slab, (((1,), (1,)), ((), ())), preferred_element_type=jnp.float32)
        integrals = integrals.astype(jnp.bfloat16).reshape(NW, V * V)
        return lax.dot_general(integrals, flat_amps, (((1,), (1,)), ((), ())), preferred_element_type=jnp.float32)

    ladder = lax.map(one_column, factors)
    counter = jnp.arange(P_SIZE, dtype=jnp.int32)
    swapped = (pair_order % NOCC) * NOCC + pair_order // NOCC
    matches = swapped[:, None] == pair_order[None, :]
    partner = jnp.sum(jnp.where(matches, counter[None, :], 0), axis=1).astype(jnp.int32)
    total = ladder + jnp.transpose(ladder, (1, 0, 2))[:, :, partner]
    virtual_energy = levels[vir_bin]
    occupied_energy = -levels[occ_bin]
    pair_energy = occupied_energy[pair_order // NOCC] + occupied_energy[pair_order % NOCC]
    denominator = virtual_energy[:, None, None] + virtual_energy[None, :, None] - pair_energy[None, None, :] + level_shift
    return (total / denominator).reshape(NW, NW * P_SIZE)
```

```python
import functools

import jax
import jax.numpy as jnp
from jax import lax
from jax.experimental import pallas as pl
from jax.experimental.pallas import tpu as pltpu
from jax.sharding import PartitionSpec as P

NOCC = 8
LANES = 128
MESH = pl.DeviceIdType.MESH

level_shift = 0.3


def flip_bits(index, bits):
    result = index
    bit = 1
    while bit <= bits:
        if bits & bit:
            result = result + bit - 2 * bit * ((result // bit) % 2)
        bit *= 2
    return result


def to_column(row):
    n = row.shape[1]
    rows = lax.broadcasted_iota(jnp.int32, (n, n), 0)
    lanes = lax.broadcasted_iota(jnp.int32, (n, n), 1)
    return jnp.sum(jnp.where(rows == lanes, row, jnp.zeros_like(row)), axis=1, keepdims=True)


def kernel(
    dims,
    f_hbm,
    amps_hbm,
    order_ref,
    occ_ref,
    vir_ref,
    levels_ref,
    out_ref,
    local,
    right,
    other,
    left_f32,
    left,
    raw,
    stage,
    amps,
    ints,
    flat,
    acc,
    tiles,
    parts,
    load_sem,
    own_sem,
    amp_sem,
    send_z,
    send_o,
    send_c,
    send_y,
    recv_piece,
    recv_y,
    send_f,
    recv_f,
):
    nz, ny, no, owned, cols, qs, window, pairs, virt, tile_c, amp_c = dims
    nd = no * 2
    nb = nz * owned
    total = nz * ny * nd
    split = window // nd
    ba, dev = lax.axis_index("ba"), lax.axis_index("dev")
    me = ba * nd + dev
    z, y = ba // ny, ba % ny
    outer, core = dev // 2, dev % 2
    partner_core = outer * 2 + 1 - core
    chunks = cols // amp_c
    half, half_z = window // 2, nz // 2
    mine = z // half_z
    halves = (mine, 1 - mine)

    load = pltpu.make_async_copy(f_hbm, local, load_sem)
    load.start()
    own = pltpu.make_async_copy(
        f_hbm.at[:, :, pl.ds(pl.multiple_of(z * qs, LANES), qs)], right.at[z, :, dev], own_sem
    )
    own.start()

    def amp_load(chunk):
        return pltpu.make_async_copy(
            amps_hbm.at[:, pl.ds(chunk * amp_c, amp_c), :], raw.at[chunk], amp_sem.at[chunk]
        )

    for chunk in range(chunks):
        amp_load(chunk).start()

    barrier = pltpu.get_barrier_semaphore()

    near = [(flip_bits(z, step) * ny + y, dev) for step in range(1, nz)]
    near += [(z * ny + flip_bits(y, step), dev) for step in range(1, ny)]
    near += [(ba, flip_bits(outer, step) * 2 + core) for step in range(1, no)]
    near.append((ba, partner_core))
    for there in near:
        pl.semaphore_signal(barrier, inc=1, device_id=there, device_id_type=MESH)
    load.wait()
    own.wait()
    pl.semaphore_wait(barrier, len(near))

    def piece_copy(piece_z, row, piece_d, send, ba_to, dev_to):
        return pltpu.make_async_remote_copy(
            src_ref=right.at[piece_z, row, piece_d],
            dst_ref=right.at[piece_z, row, piece_d],
            send_sem=send,
            recv_sem=recv_piece.at[piece_z, row, piece_d],
            device_id=(ba_to, dev_to),
            device_id_type=MESH,
        )

    def await_piece(piece_z, row, piece_d):
        piece_copy(piece_z, row, piece_d, send_z.at[0, 0], ba, partner_core).wait_recv()

    pending = []
    for step in range(1, nz):
        there = flip_bits(z, step)
        for row in range(owned):
            copy = pltpu.make_async_remote_copy(
                src_ref=local.at[row, :, pl.ds(pl.multiple_of(there * qs, LANES), qs)],
                dst_ref=right.at[z, row, dev],
                send_sem=send_z.at[step, row],
                recv_sem=recv_piece.at[z, row, dev],
                device_id=(there * ny + y, dev),
                device_id_type=MESH,
            )
            copy.start()
            pending.append(copy)

    def forward(step, row):
        from_z = flip_bits(z, step)
        if step:
            await_piece(from_z, row, dev)
        for other_outer in range(1, no):
            copy = piece_copy(
                from_z,
                row,
                dev,
                send_o.at[step, row, other_outer],
                ba,
                flip_bits(outer, other_outer) * 2 + core,
            )
            copy.start()
            pending.append(copy)
        for other_y in range(1, ny):
            copy = pltpu.make_async_remote_copy(
                src_ref=right.at[from_z, row, dev],
                dst_ref=other.at[y, from_z, row],
                send_sem=send_y.at[step, row, other_y],
                recv_sem=recv_y.at[y, from_z, row],
                device_id=(z * ny + flip_bits(y, other_y), dev),
                device_id_type=MESH,
            )
            copy.start()
            pending.append(copy)
        copy = piece_copy(from_z, row, dev, send_c.at[step, row, 0], ba, partner_core)
        copy.start()
        pending.append(copy)

    def widen(source, at_y, at_z):
        for i in range(owned):
            row = (at_z * ny + at_y) * owned + i
            base = pl.multiple_of(row * (cols + 8), 8)
            for h in range(qs // LANES):
                left_f32[h, pl.ds(base, cols), :] = source[
                    i, :, h * LANES : (h + 1) * LANES
                ].astype(jnp.float32)

    def amp_chunk(chunk):
        amp_load(chunk).wait()
        pitch = amp_c + 8

        def spread(k, carry):
            base = pl.multiple_of(k * pitch, 8)
            for h in range(virt // LANES):
                stage[h, pl.ds(base, amp_c), :] = raw[
                    chunk, k, :, h * LANES : (h + 1) * LANES
                ].astype(jnp.float32)
            return carry

        lax.fori_loop(0, pairs, spread, 0, unroll=4)

        def gather(c, carry):
            for h in range(virt // LANES):
                amps[chunk * amp_c + c, :, h * LANES : (h + 1) * LANES] = stage[
                    h, pl.ds(c, pairs, stride=pitch), :
                ].astype(jnp.bfloat16)
            return carry

        lax.fori_loop(0, amp_c, gather, 0)

    def own_rows(step):
        from_z = flip_bits(z, step)
        widen(right.at[from_z, :, dev], y, from_z)

    def collect(step):
        from_z = flip_bits(z, step)
        for row in range(owned):
            for other_outer in range(1, no):
                from_d = flip_bits(outer, other_outer) * 2 + core
                await_piece(from_z, row, from_d)
                copy = piece_copy(
                    from_z, row, from_d, send_c.at[step, row, other_outer], ba, partner_core
                )
                copy.start()
                pending.append(copy)
        for other_y in range(1, ny):
            from_y = flip_bits(y, other_y)
            for row in range(owned):
                pltpu.make_async_remote_copy(
                    src_ref=right.at[from_z, row, dev],
                    dst_ref=other.at[from_y, from_z, row],
                    send_sem=send_z.at[0, 0],
                    recv_sem=recv_y.at[from_y, from_z, row],
                    device_id=(ba, partner_core),
                    device_id_type=MESH,
                ).wait_recv()
            widen(other.at[from_y, from_z], from_y, from_z)

    def finish(step):
        from_z = flip_bits(z, step)
        for row in range(owned):
            for other_outer in range(no):
                await_piece(from_z, row, flip_bits(outer, other_outer) * 2 + 1 - core)

    def turn_half(side):
        first_row = halves[side] * half * (cols + 8)

        def turn(step, carry):
            at = step * 2
            rows = pl.ds(pl.multiple_of(at * half, 2 * half), 2 * half)
            for h in range(qs // LANES):
                left[side, rows, h * LANES : (h + 1) * LANES] = jnp.concatenate(
                    [
                        left_f32[h, pl.ds(first_row + at + i, half, stride=cols + 8), :]
                        for i in range(2)
                    ],
                    axis=0,
                ).astype(jnp.bfloat16)
            return carry

        lax.fori_loop(0, cols // 2, turn, 0, unroll=4)

    block = tile_c * half
    early = [(0, 0, j) for j in range(half_z)]
    late = [(1, side, j) for side in range(2) for j in range(half_z)] + [
        (0, 1, j) for j in range(half_z)
    ]
    height_of = owned * half

    def contract(ct, jobs, base):
        for at, (a_side, b_side, j) in enumerate(jobs):
            rows = left[a_side, pl.ds(pl.multiple_of(ct * block, block), block), :]
            from_z = halves[b_side] * half_z + j
            parts_of = []
            for i in range(owned):
                side = right[from_z, i].reshape(virt, qs)
                parts_of.append(
                    lax.dot_general(
                        rows, side, (((1,), (1,)), ((), ())), preferred_element_type=jnp.float32
                    ).reshape(tile_c, half, virt)
                )
            ints[:, at * height_of : (at + 1) * height_of, :] = jnp.concatenate(
                parts_of, axis=1
            ).astype(jnp.bfloat16)
        count = len(jobs) * height_of

        def add(t, value):
            return value + lax.dot_general(
                ints[t, 0:count, :],
                amps[ct * tile_c + t],
                (((1,), (1,)), ((), ())),
                preferred_element_type=jnp.float32,
            )

        flat[base : base + count, :] += lax.fori_loop(
            0, tile_c, add, jnp.zeros((count, pairs), jnp.float32), unroll=tile_c
        )

    flat[...] = jnp.zeros_like(flat)
    done = 0
    for step in range(half_z):
        for row in range(owned):
            forward(step, row)
            upto = (step * owned + row + 1) * chunks // (half_z * owned)
            for chunk in range(done, upto):
                amp_chunk(chunk)
            done = upto
        own_rows(step)
    for step in range(half_z, nz - 1):
        for row in range(owned):
            forward(step, row)
    for step in range(half_z):
        collect(step)
    turn_half(0)
    for step in range(half_z):
        finish(step)
    for row in range(owned):
        forward(nz - 1, row)

    def early_tile(ct, carry):
        contract(ct, early, 0)
        return carry

    lax.fori_loop(0, cols // tile_c, early_tile, 0)
    for step in range(half_z, nz):
        own_rows(step)
    for step in range(half_z, nz):
        collect(step)
    turn_half(1)
    for step in range(half_z, nz):
        finish(step)
    late_base = len(early) * height_of

    def late_tile(ct, carry):
        contract(ct, late, late_base)
        return carry

    lax.fori_loop(0, cols // tile_c, late_tile, 0)
    for at, (a_side, b_side, j) in enumerate(early + late):
        for i in range(owned):
            value = flat[at * height_of + i * half : at * height_of + (i + 1) * half, :]
            acc[
                (halves[b_side] * half_z + j) * owned + i,
                pl.ds(pl.multiple_of(halves[a_side] * half, 8), half),
                0:pairs,
            ] = value
    acc[:, :, pairs : 2 * pairs] = acc[:, :, 0:pairs]

    height = owned * split
    row_at = lax.broadcasted_iota(jnp.int32, (height, 2 * pairs), 0)
    lane_at = lax.broadcasted_iota(jnp.int32, (height, 2 * pairs), 1)

    def make_tile(there):
        to_ba, to_dev = there // nd, there % nd
        to_z, to_y = to_ba // ny, to_ba % ny
        straight = jnp.zeros((height, 2 * pairs), jnp.float32)
        pieces = []
        turned = []
        for i in range(owned):
            pieces.append(acc[to_z * owned + i, pl.ds(to_dev * split, split), :])
            for a in range(split):
                row = to_dev * split + a
                owner = row // owned
                turned.append(
                    acc[(owner // ny) * owned + row % owned, pl.ds(to_ba * owned + i, 1), :]
                )
        straight = jnp.concatenate(pieces, axis=0)
        flipped = jnp.concatenate(turned, axis=0)
        same = jnp.zeros((height, 2 * pairs), jnp.int32) + to_y == y
        owner_at = (to_dev * split + row_at % split) // owned
        return jnp.where(
            lane_at < pairs,
            jnp.where(same, straight, 0.0),
            jnp.where(owner_at % ny == y, flipped, 0.0),
        )

    def tile_copy(there):
        return pltpu.make_async_remote_copy(
            src_ref=tiles.at[there],
            dst_ref=parts.at[me],
            send_sem=send_f.at[there],
            recv_sem=recv_f.at[me],
            device_id=(there // nd, there % nd),
            device_id_type=MESH,
        )

    def send_tile(step, carry):
        there = (me + step) % total
        tiles[there] = make_tile(there)
        tile_copy(there).start()
        return carry

    lax.fori_loop(1, total, send_tile, 0)
    parts[me] = make_tile(me)

    levels = to_column(levels_ref[...])
    level_at = lax.broadcasted_iota(jnp.int32, (levels.shape[0], window), 0)
    virtual = jnp.sum(
        jnp.where(level_at == vir_ref[...], levels, 0.0), axis=0, keepdims=True
    )
    level_occ = lax.broadcasted_iota(jnp.int32, (levels.shape[0], NOCC), 0)
    occupied = to_column(
        -jnp.sum(jnp.where(level_occ == occ_ref[...], levels, 0.0), axis=0, keepdims=True)
    )
    order = order_ref[...]
    first, second = order // NOCC, order % NOCC
    occ_at = lax.broadcasted_iota(jnp.int32, (NOCC, pairs), 0)
    pair_energy = jnp.sum(
        jnp.where(occ_at == first, occupied, 0.0), axis=0, keepdims=True
    ) + jnp.sum(jnp.where(occ_at == second, occupied, 0.0), axis=0, keepdims=True)
    win_row = lax.broadcasted_iota(jnp.int32, (height, window), 0)
    win_lane = lax.broadcasted_iota(jnp.int32, (height, window), 1)
    right_energy = jnp.sum(
        jnp.where(win_lane == ba * owned + win_row // split, virtual, 0.0), axis=1, keepdims=True
    )
    left_energy = jnp.sum(
        jnp.where(win_lane == dev * split + win_row % split, virtual, 0.0), axis=1, keepdims=True
    )
    denominator = right_energy + left_energy - pair_energy + level_shift
    permuter = (to_column(order) == second * NOCC + first).astype(jnp.float32)

    def arrive(step, carry):
        there = (me + step) % total
        pltpu.make_async_remote_copy(
            src_ref=tiles.at[there],
            dst_ref=parts.at[there],
            send_sem=send_f.at[there],
            recv_sem=recv_f.at[there],
            device_id=(there // nd, there % nd),
            device_id_type=MESH,
        ).wait_recv()
        return carry

    lax.fori_loop(1, total, arrive, 0)
    summed = jnp.sum(parts[...], axis=0)
    moved = jnp.dot(
        summed[:, pairs:],
        permuter,
        precision=lax.Precision.HIGHEST,
        preferred_element_type=jnp.float32,
    )
    result = (summed[:, :pairs] + moved) / denominator
    for i in range(owned):
        for a in range(split):
            out_ref[i : i + 1, a * pairs : (a + 1) * pairs] = result[
                i * split + a : i * split + a + 1, :
            ]

    for copy in pending:
        copy.wait_send()

    def sent(step, carry):
        tile_copy((me + step) % total).wait_send()
        return carry

    lax.fori_loop(1, total, sent, 0)


def per_device(nba, ndev, factors, amplitudes, pair_order, occ_bin, vir_bin, levels):
    owned, cols, fitting = factors.shape
    pairs, _, virt = amplitudes.shape
    window = owned * nba
    ny = 1
    while ny * ny * 4 <= nba:
        ny *= 2
    nz = nba // ny
    no = ndev // 2
    qs = fitting // nz
    nb = nz * owned
    split = window // ndev
    total = nba * ndev
    tile_c = min(cols, max(1, (4 << 20) // (nb * window * virt * 2)))
    amp_c = 16
    dims = (nz, ny, no, owned, cols, qs, window, pairs, virt, tile_c, amp_c)
    dma = pltpu.SemaphoreType.DMA
    vmem = pl.BlockSpec(memory_space=pltpu.VMEM)
    hbm = pl.BlockSpec(memory_space=pl.ANY)
    return pl.pallas_call(
        functools.partial(kernel, dims),
        out_shape=jax.ShapeDtypeStruct((owned, split * pairs), jnp.float32),
        in_specs=[hbm, hbm, vmem, vmem, vmem, vmem],
        out_specs=vmem,
        scratch_shapes=[
            pltpu.VMEM((owned, cols, fitting), jnp.bfloat16),
            pltpu.VMEM((nz, owned, ndev, cols, qs), jnp.bfloat16),
            pltpu.VMEM((ny, nz, owned, cols, qs), jnp.bfloat16),
            pltpu.VMEM((qs // LANES, window * (cols + 8), LANES), jnp.float32),
            pltpu.VMEM((2, cols * window // 2, qs), jnp.bfloat16),
            pltpu.VMEM((cols // amp_c, pairs, amp_c, virt), jnp.bfloat16),
            pltpu.VMEM((virt // LANES, pairs * (amp_c + 8), LANES), jnp.float32),
            pltpu.VMEM((cols, pairs, virt), jnp.bfloat16),
            pltpu.VMEM((tile_c, nb * window, virt), jnp.bfloat16),
            pltpu.VMEM((nb * window, pairs), jnp.float32),
            pltpu.VMEM((nb, window, 2 * pairs), jnp.float32),
            pltpu.VMEM((total, owned * split, 2 * pairs), jnp.float32),
            pltpu.VMEM((total, owned * split, 2 * pairs), jnp.float32),
            dma,
            dma,
            dma((cols // amp_c,)),
            dma((nz, owned)),
            dma((nz, owned, no)),
            dma((nz, owned, no)),
            dma((nz, owned, ny)),
            dma((nz, owned, ndev)),
            dma((ny, nz, owned)),
            dma((total,)),
            dma((total,)),
        ],
        compiler_params=pltpu.CompilerParams(
            collective_id=0, has_side_effects=True, vmem_limit_bytes=56 << 20
        ),
    )(
        factors,
        amplitudes,
        pair_order.reshape(1, -1),
        occ_bin.reshape(1, -1),
        vir_bin.reshape(1, -1),
        levels.reshape(1, -1),
    )


def solution(mesh):
    return jax.shard_map(
        functools.partial(per_device, mesh.shape["ba"], mesh.shape["dev"]),
        mesh=mesh,
        in_specs=(P("ba", "dev", None), P(None, "dev", None), P(), P(), P(), P()),
        out_specs=P("ba", "dev"),
        check_vma=False,
    )
```

```python
import functools

import jax
import jax.numpy as jnp
from jax import lax
from jax.experimental import pallas as pl
from jax.experimental.pallas import tpu as pltpu
from jax.sharding import PartitionSpec as P

NOCC = 8
LANES = 128
MESH = pl.DeviceIdType.MESH

level_shift = 0.3


def flip_bits(index, bits):
    result = index
    bit = 1
    while bit <= bits:
        if bits & bit:
            result = result + bit - 2 * bit * ((result // bit) % 2)
        bit *= 2
    return result


def to_column(row):
    n = row.shape[1]
    rows = lax.broadcasted_iota(jnp.int32, (n, n), 0)
    lanes = lax.broadcasted_iota(jnp.int32, (n, n), 1)
    return jnp.sum(jnp.where(rows == lanes, row, jnp.zeros_like(row)), axis=1, keepdims=True)


def kernel(
    dims,
    f_hbm,
    amps_hbm,
    order_hbm,
    occ_hbm,
    vir_hbm,
    levels_hbm,
    out_ref,
    order_ref,
    occ_ref,
    vir_ref,
    levels_ref,
    right,
    other,
    left_f32,
    left,
    raw,
    stage,
    amps,
    ints,
    flat,
    acc,
    tiles_s,
    tiles_f,
    parts_s,
    parts_f,
    own_sem,
    small_sem,
    amp_sem,
    sent_z,
    sent_x,
    sent_y,
    sent_c,
    sent_f,
    recv_z,
    recv_x,
    recv_c,
    recv_y,
    recv_f,
):
    nz, ny, no, owned, cols, qs, window, pairs, virt, amp_c, slabs = dims
    nd = no * 2
    nb = nz * owned
    total = nz * ny * nd
    split = window // nd
    wide = cols // slabs
    ba, dev = lax.axis_index("ba"), lax.axis_index("dev")
    me = ba * nd + dev
    z, y = ba // ny, ba % ny
    outer, core = dev // 2, dev % 2
    partner_core = outer * 2 + 1 - core
    chunks = cols // amp_c

    barrier = pltpu.get_barrier_semaphore()
    near = [(flip_bits(z, step) * ny + y, dev) for step in range(1, nz)]
    near += [(z * ny + flip_bits(y, step), dev) for step in range(1, ny)]
    near += [(ba, flip_bits(outer, step) * 2 + core) for step in range(1, no)]
    near.append((ba, partner_core))
    for there in near:
        pl.semaphore_signal(barrier, inc=1, device_id=there, device_id_type=MESH)

    def quarter(at_z):
        return pl.ds(pl.multiple_of(at_z * qs, LANES), qs)

    def factor_slab(slab, at_z):
        return f_hbm.at[:, pl.ds(slab * wide, wide), quarter(at_z)]

    own = pltpu.make_async_copy(f_hbm.at[:, :, quarter(z)], right.at[z, :, dev], own_sem)
    own.start()

    def amp_load(chunk):
        return pltpu.make_async_copy(
            amps_hbm.at[:, pl.ds(chunk * amp_c, amp_c), :], raw.at[chunk], amp_sem.at[chunk]
        )

    for chunk in range(chunks):
        amp_load(chunk).start()
    small = [
        pltpu.make_async_copy(source, target, small_sem.at[at])
        for at, (source, target) in enumerate(
            (
                (order_hbm, order_ref),
                (occ_hbm, occ_ref),
                (vir_hbm, vir_ref),
                (levels_hbm, levels_ref),
            )
        )
    ]
    for copy in small:
        copy.start()
    pl.semaphore_wait(barrier, len(near))

    def send(source, target, send_sem, recv_sem, ba_to, dev_to):
        copy = pltpu.make_async_remote_copy(
            src_ref=source,
            dst_ref=target,
            send_sem=send_sem,
            recv_sem=recv_sem,
            device_id=(ba_to, dev_to),
            device_id_type=MESH,
        )
        copy.start()

    def await_bytes(place, recv_sem):
        pltpu.make_async_remote_copy(
            src_ref=place,
            dst_ref=place,
            send_sem=sent_z,
            recv_sem=recv_sem,
            device_id=(ba, partner_core),
            device_id_type=MESH,
        ).wait_recv()

    def piece(slab, at_z, at_d):
        return right.at[at_z, :, at_d, pl.ds(slab * wide, wide), :]

    def to_partner(source, slab, step, at_d):
        at_z = flip_bits(z, step)
        send(source, piece(slab, at_z, at_d), sent_c, recv_c.at[min(step // 2, 1)], ba, partner_core)

    def spread(source, slab, step):
        at_z = flip_bits(z, step)
        for other_outer in range(1, no):
            send(
                source,
                piece(slab, at_z, dev),
                sent_x,
                recv_x.at[slab, step, other_outer - 1],
                ba,
                flip_bits(outer, other_outer) * 2 + core,
            )
        for other_y in range(1, ny):
            send(
                source,
                other.at[slab, other_y - 1, at_z],
                sent_y,
                recv_y.at[slab],
                z * ny + flip_bits(y, other_y),
                dev,
            )
        to_partner(source, slab, step, dev)


    def launch(slab, steps):
        for step in steps:
            at_z = flip_bits(z, step)
            send(
                factor_slab(slab, at_z),
                piece(slab, z, dev),
                sent_z,
                recv_z.at[slab, step - 1],
                at_z * ny + y,
                dev,
            )

    def from_z(slab, step):
        place = piece(slab, flip_bits(z, step), dev)
        await_bytes(place, recv_z.at[slab, step - 1])
        spread(place, slab, step)

    def from_x(slab, step):
        for other_outer in range(1, no):
            at_d = flip_bits(outer, other_outer) * 2 + core
            place = piece(slab, flip_bits(z, step), at_d)
            await_bytes(place, recv_x.at[slab, step, other_outer - 1])
            to_partner(place, slab, step, at_d)

    def from_core(steps):
        await_bytes(right.at[0 : len(steps), :, 0:no], recv_c.at[min(steps[0] // 2, 1)])

    def widen(source, row):
        base = pl.multiple_of(row * (wide + 8), 8)
        for h in range(qs // LANES):
            left_f32[h, pl.ds(base, wide), :] = source[:, h * LANES : (h + 1) * LANES].astype(
                jnp.float32
            )

    def make_left(slab):
        if ny > 1:
            await_bytes(other.at[slab, 0 : ny - 1], recv_y.at[slab])
        for at_z in range(nz):
            for i in range(owned):
                widen(
                    right.at[at_z, i, dev, pl.ds(slab * wide, wide), :],
                    (at_z * ny + y) * owned + i,
                )
                for other_y in range(1, ny):
                    at_y = flip_bits(y, other_y)
                    widen(other.at[slab, other_y - 1, at_z, i], (at_z * ny + at_y) * owned + i)

        def turn(c, carry):
            rows = pl.ds(pl.multiple_of((slab * wide + c) * window, window), window)
            for h in range(qs // LANES):
                left[rows, h * LANES : (h + 1) * LANES] = left_f32[
                    h, pl.ds(c, window, stride=wide + 8), :
                ].astype(jnp.bfloat16)
            return carry

        lax.fori_loop(0, wide, turn, 0, unroll=wide)

    pitch = amp_c + 8

    def amp_chunk(chunk):
        amp_load(chunk).wait()
        for k in range(pairs):
            for h in range(virt // LANES):
                stage[h, k * pitch : k * pitch + amp_c, :] = raw[
                    chunk, k, :, h * LANES : (h + 1) * LANES
                ].astype(jnp.float32)
        for c in range(amp_c):
            for h in range(virt // LANES):
                amps[chunk * amp_c + c, :, h * LANES : (h + 1) * LANES] = stage[
                    h, pl.ds(c, pairs, stride=pitch), :
                ].astype(jnp.bfloat16)

    def integrals(first, count, steps):
        rows = left[first * wide * window : (first + count) * wide * window, :]
        for step in steps:
            for i in range(owned):
                side = right[flip_bits(z, step), i].reshape(virt, qs)
                at = (step * owned + i) * window
                ints[first * wide : (first + count) * wide, at : at + window, :] = (
                    lax.dot_general(
                        rows, side, (((1,), (1,)), ((), ())), preferred_element_type=jnp.float32
                    )
                    .astype(jnp.bfloat16)
                    .reshape(count * wide, window, virt)
                )

    def ladder(slab, steps):
        at, count = steps[0] * owned * window, len(steps) * owned * window
        span = range(slab * wide, (slab + 1) * wide)
        flat[at : at + count, :] += lax.dot_general(
            jnp.concatenate([ints[c, at : at + count, :] for c in span], axis=1),
            jnp.concatenate([amps[c] for c in span], axis=1),
            (((1,), (1,)), ((), ())),
            preferred_element_type=jnp.float32,
        )

    early, late = tuple(range(2)), tuple(range(2, nz))
    flat[...] = jnp.zeros_like(flat)
    own.wait()
    todo = list(range(chunks))

    def prepare(count=1):
        for chunk in todo[:count]:
            amp_chunk(chunk)
        del todo[:count]

    launch(0, range(1, nz))
    spread(factor_slab(0, z), 0, 0)
    prepare()
    for slab in range(1, slabs):
        launch(slab, (1,))
        spread(factor_slab(slab, z), slab, 0)
    prepare()
    for slab in range(1, slabs):
        launch(slab, late)
        prepare(slab % 2)
    for step in range(1, nz):
        from_z(0, step)
        prepare()
    for slab in range(1, slabs):
        from_z(slab, 1)
        from_x(slab - 1, 0)
        if slab > 1:
            prepare()
    prepare(chunks)
    from_x(slabs - 1, 0)
    for step in range(1, nz):
        from_x(0, step)
    for slab in range(1, slabs):
        from_x(slab, 1)

    def far_z(slab):
        if 0 < slab < slabs:
            for step in late:
                from_z(slab, step)

    def far_x(slab):
        if 0 < slab < slabs:
            for step in late:
                from_x(slab, step)

    far_z(1)
    for slab in range(slabs):
        make_left(slab)
        if slab == 0:
            from_core(early)
        integrals(slab, 1, early)
        if slab == 0:
            far_z(2)
        far_x(slab + 1)
        ladder(slab, early)
        if slab == 0:
            far_z(3)
    from_core(late)
    integrals(0, slabs, late)
    for slab in range(slabs):
        ladder(slab, late)

    for step in range(nz):
        for i in range(owned):
            at = (step * owned + i) * window
            acc[flip_bits(z, step) * owned + i] = flat[at : at + window, :]

    height = owned * split
    turns = split // owned
    here = z * nd + dev
    for at_z in range(nz):
        wide_row = jnp.concatenate([acc[at_z * owned + i] for i in range(owned)], axis=1)
        for at_d in range(nd):
            tiles_s[at_z, at_d] = wide_row[at_d * split : (at_d + 1) * split, :]
        for r in range(owned):
            turned = jnp.concatenate(
                [
                    acc[at_z * owned + r, pl.ds(i, window // owned, stride=owned), :]
                    for i in range(owned)
                ],
                axis=1,
            )
            for to_ba in range(window // owned):
                tiles_f[to_ba * nz + at_z, r : r + 1, :] = turned[to_ba : to_ba + 1, :]

    def post(source, target, at, to_ba, to_dev):
        there = to_ba * nd + to_dev

        @pl.when(there != me)
        def _():
            pltpu.make_async_remote_copy(
                src_ref=source,
                dst_ref=target,
                send_sem=sent_f.at[at],
                recv_sem=recv_f.at[at],
                device_id=(to_ba, to_dev),
                device_id_type=MESH,
            ).start()

        @pl.when(there == me)
        def _():
            pltpu.make_async_copy(source, target, recv_f.at[at]).start()

    def post_turned(to_ba, carry):
        for at_z in range(nz):
            owner = at_z * ny + y
            post(
                tiles_f.at[to_ba * nz + at_z],
                parts_f.at[owner % turns, here],
                1,
                to_ba,
                owner // turns,
            )
        return carry

    def post_straight(at_z, carry):
        for at_d in range(nd):
            post(tiles_s.at[at_z, at_d], parts_s.at[here], 0, at_z * ny + y, at_d)
        return carry

    if total <= 64:
        for to_ba in range(window // owned):
            if to_ba % ny == 0:
                post_straight(to_ba // ny, 0)
            post_turned(to_ba, 0)
    else:
        lax.fori_loop(0, nz, post_straight, 0)
        lax.fori_loop(0, window // owned, post_turned, 0)

    for copy in small:
        copy.wait()
    levels = to_column(levels_ref[...])
    level_at = lax.broadcasted_iota(jnp.int32, (levels.shape[0], window), 0)
    virtual = jnp.sum(
        jnp.where(level_at == vir_ref[...], levels, 0.0), axis=0, keepdims=True
    )
    level_occ = lax.broadcasted_iota(jnp.int32, (levels.shape[0], NOCC), 0)
    occupied = to_column(
        -jnp.sum(jnp.where(level_occ == occ_ref[...], levels, 0.0), axis=0, keepdims=True)
    )
    order = order_ref[...]
    first, second = order // NOCC, order % NOCC
    occ_at = lax.broadcasted_iota(jnp.int32, (NOCC, pairs), 0)
    pair_energy = jnp.sum(
        jnp.where(occ_at == first, occupied, 0.0), axis=0, keepdims=True
    ) + jnp.sum(jnp.where(occ_at == second, occupied, 0.0), axis=0, keepdims=True)
    win_row = lax.broadcasted_iota(jnp.int32, (height, window), 0)
    win_lane = lax.broadcasted_iota(jnp.int32, (height, window), 1)
    right_energy = jnp.sum(
        jnp.where(win_lane == ba * owned + win_row // split, virtual, 0.0), axis=1, keepdims=True
    )
    left_energy = jnp.sum(
        jnp.where(win_lane == dev * split + win_row % split, virtual, 0.0), axis=1, keepdims=True
    )
    denominator = right_energy + left_energy - pair_energy + level_shift
    permuter = (to_column(order) == second * NOCC + first).astype(jnp.float32)

    for at, place in enumerate((parts_s, parts_f)):
        pltpu.make_async_copy(place, place, recv_f.at[at]).wait()
    straight = jnp.sum(parts_s[...], axis=0)
    flipped = jnp.concatenate([jnp.sum(parts_f[j], axis=0) for j in range(turns)], axis=0)

    def stack(value):
        return jnp.concatenate(
            [value[:, i * pairs : (i + 1) * pairs] for i in range(owned)], axis=0
        )

    moved = jnp.dot(
        stack(flipped),
        permuter,
        precision=lax.Precision.HIGHEST,
        preferred_element_type=jnp.float32,
    )
    result = (stack(straight) + moved) / denominator
    for i in range(owned):
        for a in range(split):
            out_ref[i : i + 1, a * pairs : (a + 1) * pairs] = result[
                i * split + a : i * split + a + 1, :
            ]

    def await_sent(place, sem):
        pltpu.make_async_copy(place, place, sem).wait()

    await_sent(right.at[0 : nz - 1, :, 0], sent_z)
    await_sent(right.at[:, :, 0:no], sent_c)
    if no > 1:
        await_sent(right.at[:, :, 0 : no - 1], sent_x)
    if ny > 1:
        await_sent(other, sent_y)
    await_sent(parts_s.at[0 : nz * nd - 1], sent_f.at[0])
    kept = sum(
        jnp.where((at_z * ny + y) // turns == dev, 1, 0) for at_z in range(nz)
    )
    for count in range(2):

        @pl.when(kept == count)
        def _():
            await_sent(tiles_f.at[0 : tiles_f.shape[0] - count], sent_f.at[1])


def per_device(nba, ndev, factors, amplitudes, pair_order, occ_bin, vir_bin, levels):
    owned, cols, fitting = factors.shape
    pairs, _, virt = amplitudes.shape
    window = owned * nba
    ny = 1
    while ny * ny * 4 <= nba:
        ny *= 2
    nz = nba // ny
    no = ndev // 2
    qs = fitting // nz
    nb = nz * owned
    split = window // ndev
    amp_c = 16
    slabs = max(1, min(4, cols // 16))
    wide = cols // slabs
    dims = (nz, ny, no, owned, cols, qs, window, pairs, virt, amp_c, slabs)
    dma = pltpu.SemaphoreType.DMA
    vmem = pl.BlockSpec(memory_space=pltpu.VMEM)
    hbm = pl.BlockSpec(memory_space=pl.ANY)
    return pl.pallas_call(
        functools.partial(kernel, dims),
        out_shape=jax.ShapeDtypeStruct((owned, split * pairs), jnp.float32),
        in_specs=[hbm] * 6,
        out_specs=vmem,
        scratch_shapes=[
            pltpu.VMEM((1, pairs), jnp.int32),
            pltpu.VMEM((1, NOCC), jnp.int32),
            pltpu.VMEM((1, window), jnp.int32),
            pltpu.VMEM((1, levels.shape[0]), jnp.float32),
            pltpu.VMEM((nz, owned, ndev, cols, qs), jnp.bfloat16),
            pltpu.VMEM((slabs, max(1, ny - 1), nz, owned, wide, qs), jnp.bfloat16),
            pltpu.VMEM((qs // LANES, window * (wide + 8), LANES), jnp.float32),
            pltpu.VMEM((cols * window, qs), jnp.bfloat16),
            pltpu.VMEM((cols // amp_c, pairs, amp_c, virt), jnp.bfloat16),
            pltpu.VMEM((virt // LANES, pairs * (amp_c + 8), LANES), jnp.float32),
            pltpu.VMEM((cols, pairs, virt), jnp.bfloat16),
            pltpu.VMEM((cols, nb * window, virt), jnp.bfloat16),
            pltpu.VMEM((nb * window, pairs), jnp.float32),
            pltpu.VMEM((nb, window, pairs), jnp.float32),
            pltpu.VMEM((nz, ndev, split, owned * pairs), jnp.float32),
            pltpu.VMEM((nba * nz, owned, owned * pairs), jnp.float32),
            pltpu.VMEM((nz * ndev, split, owned * pairs), jnp.float32),
            pltpu.VMEM((split // owned, nz * ndev, owned, owned * pairs), jnp.float32),
            dma,
            dma((4,)),
            dma((cols // amp_c,)),
            dma,
            dma,
            dma,
            dma,
            dma((2,)),
            dma((slabs, nz - 1)),
            dma((slabs, nz, max(1, no - 1))),
            dma((2,)),
            dma((slabs,)),
            dma((2,)),
        ],
        compiler_params=pltpu.CompilerParams(
            collective_id=0,
            has_side_effects=True,
            vmem_limit_bytes=(63 if nb * window > 512 else 56) << 20,
        ),
    )(
        factors,
        amplitudes,
        pair_order.reshape(1, -1),
        occ_bin.reshape(1, -1),
        vir_bin.reshape(1, -1),
        levels.reshape(1, -1),
    )


def solution(mesh):
    return jax.shard_map(
        functools.partial(per_device, mesh.shape["ba"], mesh.shape["dev"]),
        mesh=mesh,
        in_specs=(P("ba", "dev", None), P(None, "dev", None), P(), P(), P(), P()),
        out_specs=P("ba", "dev"),
        check_vma=False,
    )
```

```python
import functools

import jax
import jax.numpy as jnp
from jax import lax
from jax.experimental import pallas as pl
from jax.experimental.pallas import tpu as pltpu
from jax.sharding import PartitionSpec as P

NOCC = 8
LANES = 128
MESH = pl.DeviceIdType.MESH

level_shift = 0.3


def flip_bits(index, bits):
    result = index
    bit = 1
    while bit <= bits:
        if bits & bit:
            result = result + bit - 2 * bit * ((result // bit) % 2)
        bit *= 2
    return result


def to_column(row):
    n = row.shape[1]
    rows = lax.broadcasted_iota(jnp.int32, (n, n), 0)
    lanes = lax.broadcasted_iota(jnp.int32, (n, n), 1)
    return jnp.sum(jnp.where(rows == lanes, row, jnp.zeros_like(row)), axis=1, keepdims=True)


def kernel(
    dims,
    f_hbm,
    amps_hbm,
    order_hbm,
    occ_hbm,
    vir_hbm,
    levels_hbm,
    out_ref,
    order_ref,
    occ_ref,
    vir_ref,
    levels_ref,
    right,
    other,
    left_f32,
    left,
    raw,
    stage,
    amps,
    ints,
    flat,
    acc,
    tiles_s,
    tiles_f,
    parts_s,
    parts_f,
    own_sem,
    small_sem,
    amp_sem,
    sent_z,
    sent_x,
    sent_y,
    sent_c,
    sent_f,
    recv_z,
    recv_x,
    recv_c,
    recv_y,
    recv_f,
):
    nz, ny, no, owned, cols, qs, window, pairs, virt, amp_c, slabs = dims
    nd = no * 2
    nb = nz * owned
    total = nz * ny * nd
    split = window // nd
    wide = cols // slabs
    ba, dev = lax.axis_index("ba"), lax.axis_index("dev")
    me = ba * nd + dev
    z, y = ba // ny, ba % ny
    outer, core = dev // 2, dev % 2
    partner_core = outer * 2 + 1 - core
    chunks = cols // amp_c

    barrier = pltpu.get_barrier_semaphore()
    near = [(flip_bits(z, step) * ny + y, dev) for step in range(1, nz)]
    near += [(z * ny + flip_bits(y, step), dev) for step in range(1, ny)]
    near += [(ba, flip_bits(outer, step) * 2 + core) for step in range(1, no)]
    near.append((ba, partner_core))
    for there in near:
        pl.semaphore_signal(barrier, inc=1, device_id=there, device_id_type=MESH)

    def quarter(at_z):
        return pl.ds(pl.multiple_of(at_z * qs, LANES), qs)

    def factor_slab(slab, at_z):
        return f_hbm.at[:, pl.ds(slab * wide, wide), quarter(at_z)]

    own = pltpu.make_async_copy(f_hbm.at[:, :, quarter(z)], right.at[z, :, dev], own_sem)
    own.start()

    def amp_load(chunk):
        return pltpu.make_async_copy(
            amps_hbm.at[:, pl.ds(chunk * amp_c, amp_c), :], raw.at[chunk], amp_sem.at[chunk]
        )

    for chunk in range(chunks):
        amp_load(chunk).start()
    small = [
        pltpu.make_async_copy(source, target, small_sem.at[at])
        for at, (source, target) in enumerate(
            (
                (order_hbm, order_ref),
                (occ_hbm, occ_ref),
                (vir_hbm, vir_ref),
                (levels_hbm, levels_ref),
            )
        )
    ]
    for copy in small:
        copy.start()
    pl.semaphore_wait(barrier, len(near))

    def send(source, target, send_sem, recv_sem, ba_to, dev_to):
        copy = pltpu.make_async_remote_copy(
            src_ref=source,
            dst_ref=target,
            send_sem=send_sem,
            recv_sem=recv_sem,
            device_id=(ba_to, dev_to),
            device_id_type=MESH,
        )
        copy.start()

    def await_bytes(place, recv_sem):
        pltpu.make_async_remote_copy(
            src_ref=place,
            dst_ref=place,
            send_sem=sent_z,
            recv_sem=recv_sem,
            device_id=(ba, partner_core),
            device_id_type=MESH,
        ).wait_recv()

    def piece(slab, at_z, at_d):
        return right.at[at_z, :, at_d, pl.ds(slab * wide, wide), :]

    def to_partner(source, slab, step, at_d):
        at_z = flip_bits(z, step)
        send(source, piece(slab, at_z, at_d), sent_c, recv_c.at[min(step // 2, 1)], ba, partner_core)

    def source_of(slab, step):
        return piece(slab, flip_bits(z, step), dev) if step else factor_slab(slab, z)

    def spread_x(slab, step):
        source = source_of(slab, step)
        for other_outer in range(1, no):
            send(
                source,
                piece(slab, flip_bits(z, step), dev),
                sent_x,
                recv_x.at[slab, step, other_outer - 1],
                ba,
                flip_bits(outer, other_outer) * 2 + core,
            )
        to_partner(source, slab, step, dev)

    def spread_y(slab, step):
        for other_y in range(1, ny):
            send(
                source_of(slab, step),
                other.at[slab, other_y - 1, flip_bits(z, step)],
                sent_y,
                recv_y.at[slab],
                z * ny + flip_bits(y, other_y),
                dev,
            )

    def launch(slab, steps):
        for step in steps:
            at_z = flip_bits(z, step)
            send(
                factor_slab(slab, at_z),
                piece(slab, z, dev),
                sent_z,
                recv_z.at[slab, step - 1],
                at_z * ny + y,
                dev,
            )

    def land(slab, step):
        await_bytes(piece(slab, flip_bits(z, step), dev), recv_z.at[slab, step - 1])

    def from_z(slab, step):
        land(slab, step)
        spread_y(slab, step)
        spread_x(slab, step)

    def from_x(slab, step):
        for other_outer in range(1, no):
            at_d = flip_bits(outer, other_outer) * 2 + core
            place = piece(slab, flip_bits(z, step), at_d)
            await_bytes(place, recv_x.at[slab, step, other_outer - 1])
            to_partner(place, slab, step, at_d)

    def from_core(steps):
        await_bytes(right.at[0 : len(steps), :, 0:no], recv_c.at[min(steps[0] // 2, 1)])

    def widen(source, row):
        base = pl.multiple_of(row * (wide + 8), 8)
        for h in range(qs // LANES):
            left_f32[h, pl.ds(base, wide), :] = source[:, h * LANES : (h + 1) * LANES].astype(
                jnp.float32
            )

    def make_left(slab):
        if ny > 1:
            await_bytes(other.at[slab, 0 : ny - 1], recv_y.at[slab])
        for at_z in range(nz):
            for i in range(owned):
                widen(
                    right.at[at_z, i, dev, pl.ds(slab * wide, wide), :],
                    (at_z * ny + y) * owned + i,
                )
                for other_y in range(1, ny):
                    at_y = flip_bits(y, other_y)
                    widen(other.at[slab, other_y - 1, at_z, i], (at_z * ny + at_y) * owned + i)

        def turn(c, carry):
            rows = pl.ds(pl.multiple_of((slab * wide + c) * window, window), window)
            for h in range(qs // LANES):
                left[rows, h * LANES : (h + 1) * LANES] = left_f32[
                    h, pl.ds(c, window, stride=wide + 8), :
                ].astype(jnp.bfloat16)
            return carry

        lax.fori_loop(0, wide, turn, 0, unroll=wide)

    pitch = amp_c + 8

    def amp_chunk(chunk):
        amp_load(chunk).wait()
        for k in range(pairs):
            for h in range(virt // LANES):
                stage[h, k * pitch : k * pitch + amp_c, :] = raw[
                    chunk, k, :, h * LANES : (h + 1) * LANES
                ].astype(jnp.float32)
        for c in range(amp_c):
            for h in range(virt // LANES):
                amps[chunk * amp_c + c, :, h * LANES : (h + 1) * LANES] = stage[
                    h, pl.ds(c, pairs, stride=pitch), :
                ].astype(jnp.bfloat16)

    def integrals(first, count, steps):
        rows = left[first * wide * window : (first + count) * wide * window, :]
        for step in steps:
            for i in range(owned):
                side = right[flip_bits(z, step), i].reshape(virt, qs)
                at = (step * owned + i) * window
                ints[first * wide : (first + count) * wide, at : at + window, :] = (
                    lax.dot_general(
                        rows, side, (((1,), (1,)), ((), ())), preferred_element_type=jnp.float32
                    )
                    .astype(jnp.bfloat16)
                    .reshape(count * wide, window, virt)
                )

    def ladder(slab, steps):
        at, count = steps[0] * owned * window, len(steps) * owned * window
        span = range(slab * wide, (slab + 1) * wide)
        flat[at : at + count, :] += lax.dot_general(
            jnp.concatenate([ints[c, at : at + count, :] for c in span], axis=1),
            jnp.concatenate([amps[c] for c in span], axis=1),
            (((1,), (1,)), ((), ())),
            preferred_element_type=jnp.float32,
        )

    early, late = tuple(range(2)), tuple(range(2, nz))
    todo = list(range(chunks))

    def prepare(count=1):
        for chunk in todo[:count]:
            amp_chunk(chunk)
        del todo[:count]

    @pl.when(core == 1)
    def _():
        flat[0:8, :] = lax.fori_loop(
            0, 80, lambda at, value: value * 0.5 + 1.0, jnp.zeros((8, pairs), jnp.float32)
        )

    launch(0, (1,))
    for slab in range(1, min(2, slabs)):
        launch(slab, (1,))
    spread_x(0, 0)
    spread_y(0, 0)
    launch(0, late[:-1])
    prepare()
    for slab in range(2, slabs):
        launch(slab, (1,))
        if slab == 2:
            launch(0, late[-1:])
        spread_x(slab - 1, 0)
    if slabs < 3:
        launch(0, late[-1:])
    if slabs > 1:
        spread_x(slabs - 1, 0)
        spread_y(1, 0)
    prepare()
    for slab in range(1, slabs):
        launch(slab, late)
        prepare(slab % 2)
    flat[...] = jnp.zeros_like(flat)
    own.wait()
    from_z(0, 1)
    prepare()
    if slabs > 1:
        from_z(1, 1)
        prepare()
    from_x(0, 0)
    for step in late[:-1]:
        land(0, step)
        spread_y(0, step)
        prepare()
    for slab in range(2, slabs):
        land(slab, 1)
        spread_x(slab, 1)
        from_x(slab - 1, 0)
        prepare()
    land(0, nz - 1)
    spread_y(0, nz - 1)
    if slabs > 1:
        from_x(slabs - 1, 0)
    for step in late:
        spread_x(0, step)
    for slab in range(2, slabs):
        spread_y(slab, 0)
    prepare(chunks)
    for slab in range(slabs):
        from_x(slab, 1)

    def far_z(slab):
        if 0 < slab < slabs:
            for step in late:
                land(slab, step)
                spread_y(slab, step)
            for step in late:
                spread_x(slab, step)

    def far_x(slab):
        if slab < slabs:
            for step in late:
                from_x(slab, step)

    far_z(1)
    for slab in range(2, slabs):
        spread_y(slab, 1)
    for slab in range(slabs):
        make_left(slab)
        if slab == 0:
            from_core(early)
        integrals(slab, 1, early)
        if slab > 1:
            far_x(slab)
        ladder(slab, early)
        far_z(slab + 2)
        if slab < 2:
            far_x(slab)
    from_core(late)
    integrals(0, slabs, late)
    for slab in range(slabs):
        ladder(slab, late)

    for step in range(nz):
        for i in range(owned):
            at = (step * owned + i) * window
            acc[flip_bits(z, step) * owned + i] = flat[at : at + window, :]

    height = owned * split
    turns = split // owned
    here = z * nd + dev
    for at_z in range(nz):
        wide_row = jnp.concatenate([acc[at_z * owned + i] for i in range(owned)], axis=1)
        for at_d in range(nd):
            tiles_s[at_z, at_d] = wide_row[at_d * split : (at_d + 1) * split, :]
        for r in range(owned):
            turned = jnp.concatenate(
                [
                    acc[at_z * owned + r, pl.ds(i, window // owned, stride=owned), :]
                    for i in range(owned)
                ],
                axis=1,
            )
            for to_ba in range(window // owned):
                tiles_f[to_ba * nz + at_z, r : r + 1, :] = turned[to_ba : to_ba + 1, :]

    def post(source, target, at, to_ba, to_dev):
        there = to_ba * nd + to_dev

        @pl.when(there != me)
        def _():
            pltpu.make_async_remote_copy(
                src_ref=source,
                dst_ref=target,
                send_sem=sent_f.at[at],
                recv_sem=recv_f.at[at],
                device_id=(to_ba, to_dev),
                device_id_type=MESH,
            ).start()

        @pl.when(there == me)
        def _():
            pltpu.make_async_copy(source, target, recv_f.at[at]).start()

    def post_turned(to_ba, carry):
        for at_z in range(nz):
            owner = at_z * ny + y
            post(
                tiles_f.at[to_ba * nz + at_z],
                parts_f.at[owner % turns, here],
                1,
                to_ba,
                owner // turns,
            )
        return carry

    def post_straight(at_z, carry):
        for at_d in range(nd):
            post(tiles_s.at[at_z, at_d], parts_s.at[here], 0, at_z * ny + y, at_d)
        return carry

    if total <= 64:
        for to_ba in range(window // owned):
            if to_ba % ny == 0:
                post_straight(to_ba // ny, 0)
            post_turned(to_ba, 0)
    else:
        lax.fori_loop(0, nz, post_straight, 0)
        lax.fori_loop(0, window // owned, post_turned, 0)

    for copy in small:
        copy.wait()
    levels = to_column(levels_ref[...])
    level_at = lax.broadcasted_iota(jnp.int32, (levels.shape[0], window), 0)
    virtual = jnp.sum(
        jnp.where(level_at == vir_ref[...], levels, 0.0), axis=0, keepdims=True
    )
    level_occ = lax.broadcasted_iota(jnp.int32, (levels.shape[0], NOCC), 0)
    occupied = to_column(
        -jnp.sum(jnp.where(level_occ == occ_ref[...], levels, 0.0), axis=0, keepdims=True)
    )
    order = order_ref[...]
    first, second = order // NOCC, order % NOCC
    occ_at = lax.broadcasted_iota(jnp.int32, (NOCC, pairs), 0)
    pair_energy = jnp.sum(
        jnp.where(occ_at == first, occupied, 0.0), axis=0, keepdims=True
    ) + jnp.sum(jnp.where(occ_at == second, occupied, 0.0), axis=0, keepdims=True)
    win_row = lax.broadcasted_iota(jnp.int32, (height, window), 0)
    win_lane = lax.broadcasted_iota(jnp.int32, (height, window), 1)
    right_energy = jnp.sum(
        jnp.where(win_lane == ba * owned + win_row // split, virtual, 0.0), axis=1, keepdims=True
    )
    left_energy = jnp.sum(
        jnp.where(win_lane == dev * split + win_row % split, virtual, 0.0), axis=1, keepdims=True
    )
    denominator = right_energy + left_energy - pair_energy + level_shift
    permuter = (to_column(order) == second * NOCC + first).astype(jnp.float32)

    for at, place in enumerate((parts_s, parts_f)):
        pltpu.make_async_copy(place, place, recv_f.at[at]).wait()
    straight = jnp.sum(parts_s[...], axis=0)
    flipped = jnp.concatenate([jnp.sum(parts_f[j], axis=0) for j in range(turns)], axis=0)

    def stack(value):
        return jnp.concatenate(
            [value[:, i * pairs : (i + 1) * pairs] for i in range(owned)], axis=0
        )

    moved = jnp.dot(
        stack(flipped),
        permuter,
        precision=lax.Precision.HIGHEST,
        preferred_element_type=jnp.float32,
    )
    result = (stack(straight) + moved) / denominator
    for i in range(owned):
        for a in range(split):
            out_ref[i : i + 1, a * pairs : (a + 1) * pairs] = result[
                i * split + a : i * split + a + 1, :
            ]

    def await_sent(place, sem):
        pltpu.make_async_copy(place, place, sem).wait()

    await_sent(right.at[0 : nz - 1, :, 0], sent_z)
    await_sent(right.at[:, :, 0:no], sent_c)
    if no > 1:
        await_sent(right.at[:, :, 0 : no - 1], sent_x)
    if ny > 1:
        await_sent(other, sent_y)
    await_sent(parts_s.at[0 : nz * nd - 1], sent_f.at[0])
    kept = sum(
        jnp.where((at_z * ny + y) // turns == dev, 1, 0) for at_z in range(nz)
    )
    for count in range(2):

        @pl.when(kept == count)
        def _():
            await_sent(tiles_f.at[0 : tiles_f.shape[0] - count], sent_f.at[1])


def per_device(nba, ndev, factors, amplitudes, pair_order, occ_bin, vir_bin, levels):
    owned, cols, fitting = factors.shape
    pairs, _, virt = amplitudes.shape
    window = owned * nba
    ny = 1
    while ny * ny * 4 <= nba:
        ny *= 2
    nz = nba // ny
    no = ndev // 2
    qs = fitting // nz
    nb = nz * owned
    split = window // ndev
    amp_c = 16
    slabs = max(1, min(4, cols // 16))
    wide = cols // slabs
    dims = (nz, ny, no, owned, cols, qs, window, pairs, virt, amp_c, slabs)
    dma = pltpu.SemaphoreType.DMA
    vmem = pl.BlockSpec(memory_space=pltpu.VMEM)
    hbm = pl.BlockSpec(memory_space=pl.ANY)
    return pl.pallas_call(
        functools.partial(kernel, dims),
        out_shape=jax.ShapeDtypeStruct((owned, split * pairs), jnp.float32),
        in_specs=[hbm] * 6,
        out_specs=vmem,
        scratch_shapes=[
            pltpu.VMEM((1, pairs), jnp.int32),
            pltpu.VMEM((1, NOCC), jnp.int32),
            pltpu.VMEM((1, window), jnp.int32),
            pltpu.VMEM((1, levels.shape[0]), jnp.float32),
            pltpu.VMEM((nz, owned, ndev, cols, qs), jnp.bfloat16),
            pltpu.VMEM((slabs, max(1, ny - 1), nz, owned, wide, qs), jnp.bfloat16),
            pltpu.VMEM((qs // LANES, window * (wide + 8), LANES), jnp.float32),
            pltpu.VMEM((cols * window, qs), jnp.bfloat16),
            pltpu.VMEM((cols // amp_c, pairs, amp_c, virt), jnp.bfloat16),
            pltpu.VMEM((virt // LANES, pairs * (amp_c + 8), LANES), jnp.float32),
            pltpu.VMEM((cols, pairs, virt), jnp.bfloat16),
            pltpu.VMEM((cols, nb * window, virt), jnp.bfloat16),
            pltpu.VMEM((nb * window, pairs), jnp.float32),
            pltpu.VMEM((nb, window, pairs), jnp.float32),
            pltpu.VMEM((nz, ndev, split, owned * pairs), jnp.float32),
            pltpu.VMEM((nba * nz, owned, owned * pairs), jnp.float32),
            pltpu.VMEM((nz * ndev, split, owned * pairs), jnp.float32),
            pltpu.VMEM((split // owned, nz * ndev, owned, owned * pairs), jnp.float32),
            dma,
            dma((4,)),
            dma((cols // amp_c,)),
            dma,
            dma,
            dma,
            dma,
            dma((2,)),
            dma((slabs, nz - 1)),
            dma((slabs, nz, max(1, no - 1))),
            dma((2,)),
            dma((slabs,)),
            dma((2,)),
        ],
        compiler_params=pltpu.CompilerParams(
            collective_id=0,
            has_side_effects=True,
            vmem_limit_bytes=(63 if nb * window > 512 else 56) << 20,
        ),
    )(
        factors,
        amplitudes,
        pair_order.reshape(1, -1),
        occ_bin.reshape(1, -1),
        vir_bin.reshape(1, -1),
        levels.reshape(1, -1),
    )


def solution(mesh):
    return jax.shard_map(
        functools.partial(per_device, mesh.shape["ba"], mesh.shape["dev"]),
        mesh=mesh,
        in_specs=(P("ba", "dev", None), P(None, "dev", None), P(), P(), P(), P()),
        out_specs=P("ba", "dev"),
        check_vma=False,
    )
```

```python
import functools

import jax
import jax.numpy as jnp
from jax import lax
from jax.experimental import pallas as pl
from jax.experimental.pallas import tpu as pltpu
from jax.sharding import PartitionSpec as P

NOCC = 8
LANES = 128
MESH = pl.DeviceIdType.MESH

level_shift = 0.3


def flip_bits(index, bits):
    result = index
    bit = 1
    while bit <= bits:
        if bits & bit:
            result = result + bit - 2 * bit * ((result // bit) % 2)
        bit *= 2
    return result


def to_column(row):
    n = row.shape[1]
    rows = lax.broadcasted_iota(jnp.int32, (n, n), 0)
    lanes = lax.broadcasted_iota(jnp.int32, (n, n), 1)
    return jnp.sum(jnp.where(rows == lanes, row, jnp.zeros_like(row)), axis=1, keepdims=True)


def kernel(
    dims,
    f_hbm,
    amps_hbm,
    order_hbm,
    occ_hbm,
    vir_hbm,
    levels_hbm,
    out_ref,
    order_ref,
    occ_ref,
    vir_ref,
    levels_ref,
    right,
    other,
    left_f32,
    left,
    raw,
    stage,
    amps,
    ints,
    flat,
    acc,
    tiles_s,
    tiles_f,
    parts_s,
    parts_f,
    own_sem,
    small_sem,
    amp_sem,
    sent_z,
    sent_x,
    sent_y,
    sent_c,
    sent_f,
    recv_z,
    recv_x,
    recv_c,
    recv_y,
    recv_f,
):
    nz, ny, no, owned, cols, qs, window, pairs, virt, amp_c, slabs = dims
    nd = no * 2
    nb = nz * owned
    total = nz * ny * nd
    split = window // nd
    wide = cols // slabs
    ba, dev = lax.axis_index("ba"), lax.axis_index("dev")
    me = ba * nd + dev
    z, y = ba // ny, ba % ny
    outer, core = dev // 2, dev % 2
    partner_core = outer * 2 + 1 - core
    chunks = cols // amp_c

    barrier = pltpu.get_barrier_semaphore()
    near = [(flip_bits(z, step) * ny + y, dev) for step in range(1, nz)]
    near += [(z * ny + flip_bits(y, step), dev) for step in range(1, ny)]
    near += [(ba, flip_bits(outer, step) * 2 + core) for step in range(1, no)]
    near.append((ba, partner_core))
    for there in near:
        pl.semaphore_signal(barrier, inc=1, device_id=there, device_id_type=MESH)

    def quarter(at_z):
        return pl.ds(pl.multiple_of(at_z * qs, LANES), qs)

    def factor_slab(slab, at_z):
        return f_hbm.at[:, pl.ds(slab * wide, wide), quarter(at_z)]

    own = pltpu.make_async_copy(f_hbm.at[:, :, quarter(z)], right.at[z, :, dev], own_sem)
    own.start()

    def amp_load(chunk):
        return pltpu.make_async_copy(
            amps_hbm.at[:, pl.ds(chunk * amp_c, amp_c), :], raw.at[chunk], amp_sem.at[chunk]
        )

    for chunk in range(chunks):
        amp_load(chunk).start()
    small = [
        pltpu.make_async_copy(source, target, small_sem.at[at])
        for at, (source, target) in enumerate(
            (
                (order_hbm, order_ref),
                (occ_hbm, occ_ref),
                (vir_hbm, vir_ref),
                (levels_hbm, levels_ref),
            )
        )
    ]
    for copy in small:
        copy.start()
    pl.semaphore_wait(barrier, len(near))

    def send(source, target, send_sem, recv_sem, ba_to, dev_to):
        copy = pltpu.make_async_remote_copy(
            src_ref=source,
            dst_ref=target,
            send_sem=send_sem,
            recv_sem=recv_sem,
            device_id=(ba_to, dev_to),
            device_id_type=MESH,
        )
        copy.start()

    def await_bytes(place, recv_sem):
        pltpu.make_async_remote_copy(
            src_ref=place,
            dst_ref=place,
            send_sem=sent_z,
            recv_sem=recv_sem,
            device_id=(ba, partner_core),
            device_id_type=MESH,
        ).wait_recv()

    def piece(slab, at_z, at_d):
        return right.at[at_z, :, at_d, pl.ds(slab * wide, wide), :]

    def to_partner(source, slab, step, at_d):
        at_z = flip_bits(z, step)
        send(source, piece(slab, at_z, at_d), sent_c, recv_c.at[min(step // 2, 1)], ba, partner_core)

    def source_of(slab, step):
        return piece(slab, flip_bits(z, step), dev) if step else factor_slab(slab, z)

    def spread_x(slab, step):
        source = source_of(slab, step)
        for other_outer in range(1, no):
            send(
                source,
                piece(slab, flip_bits(z, step), dev),
                sent_x,
                recv_x.at[slab, step, other_outer - 1],
                ba,
                flip_bits(outer, other_outer) * 2 + core,
            )
        to_partner(source, slab, step, dev)

    def spread_y(slab, step):
        for other_y in range(1, ny):
            send(
                source_of(slab, step),
                other.at[slab, other_y - 1, flip_bits(z, step)],
                sent_y,
                recv_y.at[slab],
                z * ny + flip_bits(y, other_y),
                dev,
            )

    def launch(slab, steps):
        for step in steps:
            at_z = flip_bits(z, step)
            send(
                factor_slab(slab, at_z),
                piece(slab, z, dev),
                sent_z,
                recv_z.at[slab, step - 1],
                at_z * ny + y,
                dev,
            )

    def land(slab, step):
        await_bytes(piece(slab, flip_bits(z, step), dev), recv_z.at[slab, step - 1])

    def from_z(slab, step):
        land(slab, step)
        spread_y(slab, step)
        spread_x(slab, step)

    def from_x(slab, step):
        for other_outer in range(1, no):
            at_d = flip_bits(outer, other_outer) * 2 + core
            place = piece(slab, flip_bits(z, step), at_d)
            await_bytes(place, recv_x.at[slab, step, other_outer - 1])
            to_partner(place, slab, step, at_d)

    def from_core(steps):
        await_bytes(right.at[0 : len(steps), :, 0:no], recv_c.at[min(steps[0] // 2, 1)])

    def widen(source, row):
        base = pl.multiple_of(row * (wide + 8), 8)
        for h in range(qs // LANES):
            left_f32[h, pl.ds(base, wide), :] = source[:, h * LANES : (h + 1) * LANES].astype(
                jnp.float32
            )

    def make_left(slab):
        if ny > 1:
            await_bytes(other.at[slab, 0 : ny - 1], recv_y.at[slab])
        for at_z in range(nz):
            for i in range(owned):
                widen(
                    right.at[at_z, i, dev, pl.ds(slab * wide, wide), :],
                    (at_z * ny + y) * owned + i,
                )
                for other_y in range(1, ny):
                    at_y = flip_bits(y, other_y)
                    widen(other.at[slab, other_y - 1, at_z, i], (at_z * ny + at_y) * owned + i)

        def turn(c, carry):
            rows = pl.ds(pl.multiple_of((slab * wide + c) * window, window), window)
            for h in range(qs // LANES):
                left[rows, h * LANES : (h + 1) * LANES] = left_f32[
                    h, pl.ds(c, window, stride=wide + 8), :
                ].astype(jnp.bfloat16)
            return carry

        lax.fori_loop(0, wide, turn, 0, unroll=wide)

    pitch = amp_c + 8

    def amp_chunk(chunk):
        amp_load(chunk).wait()
        for k in range(pairs):
            for h in range(virt // LANES):
                stage[h, k * pitch : k * pitch + amp_c, :] = raw[
                    chunk, k, :, h * LANES : (h + 1) * LANES
                ].astype(jnp.float32)
        for c in range(amp_c):
            for h in range(virt // LANES):
                amps[chunk * amp_c + c, :, h * LANES : (h + 1) * LANES] = stage[
                    h, pl.ds(c, pairs, stride=pitch), :
                ].astype(jnp.bfloat16)

    def integrals(first, count, steps):
        rows = left[first * wide * window : (first + count) * wide * window, :]
        for step in steps:
            for i in range(owned):
                side = right[flip_bits(z, step), i].reshape(virt, qs)
                at = (step * owned + i) * window
                ints[first * wide : (first + count) * wide, at : at + window, :] = (
                    lax.dot_general(
                        rows, side, (((1,), (1,)), ((), ())), preferred_element_type=jnp.float32
                    )
                    .astype(jnp.bfloat16)
                    .reshape(count * wide, window, virt)
                )

    def ladder(slab, steps):
        at, count = steps[0] * owned * window, len(steps) * owned * window
        span = range(slab * wide, (slab + 1) * wide)
        flat[at : at + count, :] += lax.dot_general(
            jnp.concatenate([ints[c, at : at + count, :] for c in span], axis=1),
            jnp.concatenate([amps[c] for c in span], axis=1),
            (((1,), (1,)), ((), ())),
            preferred_element_type=jnp.float32,
        )

    early, late = tuple(range(2)), tuple(range(2, nz))
    todo = list(range(chunks))

    def prepare(count=1):
        for chunk in todo[:count]:
            amp_chunk(chunk)
        del todo[:count]

    @pl.when(core == 1)
    def _():
        flat[0:8, :] = lax.fori_loop(
            0, 80, lambda at, value: value * 0.5 + 1.0, jnp.zeros((8, pairs), jnp.float32)
        )

    launch(0, (1,))
    for slab in range(1, min(2, slabs)):
        launch(slab, (1,))
    spread_x(0, 0)
    spread_y(0, 0)
    launch(0, late[:-1])
    prepare()
    for slab in range(2, slabs):
        launch(slab, (1,))
        if slab == 2:
            launch(0, late[-1:])
        spread_x(slab - 1, 0)
    if slabs < 3:
        launch(0, late[-1:])
    if slabs > 1:
        spread_x(slabs - 1, 0)
        spread_y(1, 0)
    prepare()
    for slab in range(1, slabs):
        launch(slab, late)
        prepare(slab % 2)
    flat[...] = jnp.zeros_like(flat)
    own.wait()
    from_z(0, 1)
    prepare()
    if slabs > 1:
        from_z(1, 1)
        prepare()
    from_x(0, 0)
    for step in late[:-1]:
        land(0, step)
        spread_y(0, step)
        prepare()
    for slab in range(2, slabs):
        land(slab, 1)
        spread_x(slab, 1)
        from_x(slab - 1, 0)
        prepare()
    land(0, nz - 1)
    spread_y(0, nz - 1)
    if slabs > 1:
        from_x(slabs - 1, 0)
    for step in late:
        spread_x(0, step)
    for slab in range(2, slabs):
        spread_y(slab, 0)
    prepare(chunks)
    for slab in range(slabs):
        if slabs > 1 and slab == slabs - 2:
            for step in late[:-1]:
                land(1, step)
                spread_y(1, step)
        if slabs > 1 and slab == slabs - 1:
            land(1, nz - 1)
            spread_y(1, nz - 1)
        from_x(slab, 1)

    def far_z(slab):
        if 0 < slab < slabs:
            for step in late:
                land(slab, step)
                spread_y(slab, step)
            for step in late:
                spread_x(slab, step)

    def far_x(slab):
        if slab < slabs:
            for step in late:
                from_x(slab, step)

    if slabs > 1:
        for step in late:
            spread_x(1, step)
    for slab in range(2, slabs):
        spread_y(slab, 1)
    for slab in range(slabs):
        make_left(slab)
        if slab == 0:
            from_core(early)
        integrals(slab, 1, early)
        if slab > 1:
            far_x(slab)
        far_z(slab + 2)
        ladder(slab, early)
        if slab < 2:
            far_x(slab)
    from_core(late)
    integrals(0, slabs, late)
    for slab in range(slabs):
        ladder(slab, late)

    for step in range(nz):
        for i in range(owned):
            at = (step * owned + i) * window
            acc[flip_bits(z, step) * owned + i] = flat[at : at + window, :]

    height = owned * split
    turns = split // owned
    here = z * nd + dev
    for at_z in range(nz):
        wide_row = jnp.concatenate([acc[at_z * owned + i] for i in range(owned)], axis=1)
        for at_d in range(nd):
            tiles_s[at_z, at_d] = wide_row[at_d * split : (at_d + 1) * split, :]
        for r in range(owned):
            turned = jnp.concatenate(
                [
                    acc[at_z * owned + r, pl.ds(i, window // owned, stride=owned), :]
                    for i in range(owned)
                ],
                axis=1,
            )
            for to_ba in range(window // owned):
                tiles_f[to_ba * nz + at_z, r : r + 1, :] = turned[to_ba : to_ba + 1, :]

    def post(source, target, at, to_ba, to_dev):
        there = to_ba * nd + to_dev

        @pl.when(there != me)
        def _():
            pltpu.make_async_remote_copy(
                src_ref=source,
                dst_ref=target,
                send_sem=sent_f.at[at],
                recv_sem=recv_f.at[at],
                device_id=(to_ba, to_dev),
                device_id_type=MESH,
            ).start()

        @pl.when(there == me)
        def _():
            pltpu.make_async_copy(source, target, recv_f.at[at]).start()

    def post_turned(to_ba, carry):
        for at_z in range(nz):
            owner = at_z * ny + y
            post(
                tiles_f.at[to_ba * nz + at_z],
                parts_f.at[owner % turns, here],
                1,
                to_ba,
                owner // turns,
            )
        return carry

    def post_straight(at_z, carry):
        for at_d in range(nd):
            post(tiles_s.at[at_z, at_d], parts_s.at[here], 0, at_z * ny + y, at_d)
        return carry

    if total <= 64:
        for to_ba in range(window // owned):
            if to_ba % ny == 0:
                post_straight(to_ba // ny, 0)
            post_turned(to_ba, 0)
    else:
        lax.fori_loop(0, nz, post_straight, 0)
        lax.fori_loop(0, window // owned, post_turned, 0)

    for copy in small:
        copy.wait()
    levels = to_column(levels_ref[...])
    level_at = lax.broadcasted_iota(jnp.int32, (levels.shape[0], window), 0)
    virtual = jnp.sum(
        jnp.where(level_at == vir_ref[...], levels, 0.0), axis=0, keepdims=True
    )
    level_occ = lax.broadcasted_iota(jnp.int32, (levels.shape[0], NOCC), 0)
    occupied = to_column(
        -jnp.sum(jnp.where(level_occ == occ_ref[...], levels, 0.0), axis=0, keepdims=True)
    )
    order = order_ref[...]
    first, second = order // NOCC, order % NOCC
    occ_at = lax.broadcasted_iota(jnp.int32, (NOCC, pairs), 0)
    pair_energy = jnp.sum(
        jnp.where(occ_at == first, occupied, 0.0), axis=0, keepdims=True
    ) + jnp.sum(jnp.where(occ_at == second, occupied, 0.0), axis=0, keepdims=True)
    win_row = lax.broadcasted_iota(jnp.int32, (height, window), 0)
    win_lane = lax.broadcasted_iota(jnp.int32, (height, window), 1)
    right_energy = jnp.sum(
        jnp.where(win_lane == ba * owned + win_row // split, virtual, 0.0), axis=1, keepdims=True
    )
    left_energy = jnp.sum(
        jnp.where(win_lane == dev * split + win_row % split, virtual, 0.0), axis=1, keepdims=True
    )
    denominator = right_energy + left_energy - pair_energy + level_shift
    permuter = (to_column(order) == second * NOCC + first).astype(jnp.float32)

    for at, place in enumerate((parts_s, parts_f)):
        pltpu.make_async_copy(place, place, recv_f.at[at]).wait()
    straight = jnp.sum(parts_s[...], axis=0)
    flipped = jnp.concatenate([jnp.sum(parts_f[j], axis=0) for j in range(turns)], axis=0)

    def stack(value):
        return jnp.concatenate(
            [value[:, i * pairs : (i + 1) * pairs] for i in range(owned)], axis=0
        )

    moved = jnp.dot(
        stack(flipped),
        permuter,
        precision=lax.Precision.HIGHEST,
        preferred_element_type=jnp.float32,
    )
    result = (stack(straight) + moved) / denominator
    for i in range(owned):
        for a in range(split):
            out_ref[i : i + 1, a * pairs : (a + 1) * pairs] = result[
                i * split + a : i * split + a + 1, :
            ]

    def await_sent(place, sem):
        pltpu.make_async_copy(place, place, sem).wait()

    await_sent(right.at[0 : nz - 1, :, 0], sent_z)
    await_sent(right.at[:, :, 0:no], sent_c)
    if no > 1:
        await_sent(right.at[:, :, 0 : no - 1], sent_x)
    if ny > 1:
        await_sent(other, sent_y)
    await_sent(parts_s.at[0 : nz * nd - 1], sent_f.at[0])
    kept = sum(
        jnp.where((at_z * ny + y) // turns == dev, 1, 0) for at_z in range(nz)
    )
    for count in range(2):

        @pl.when(kept == count)
        def _():
            await_sent(tiles_f.at[0 : tiles_f.shape[0] - count], sent_f.at[1])


def per_device(nba, ndev, factors, amplitudes, pair_order, occ_bin, vir_bin, levels):
    owned, cols, fitting = factors.shape
    pairs, _, virt = amplitudes.shape
    window = owned * nba
    ny = 1
    while ny * ny * 4 <= nba:
        ny *= 2
    nz = nba // ny
    no = ndev // 2
    qs = fitting // nz
    nb = nz * owned
    split = window // ndev
    amp_c = 16
    slabs = max(1, min(4, cols // 16))
    wide = cols // slabs
    dims = (nz, ny, no, owned, cols, qs, window, pairs, virt, amp_c, slabs)
    dma = pltpu.SemaphoreType.DMA
    vmem = pl.BlockSpec(memory_space=pltpu.VMEM)
    hbm = pl.BlockSpec(memory_space=pl.ANY)
    return pl.pallas_call(
        functools.partial(kernel, dims),
        out_shape=jax.ShapeDtypeStruct((owned, split * pairs), jnp.float32),
        in_specs=[hbm] * 6,
        out_specs=vmem,
        scratch_shapes=[
            pltpu.VMEM((1, pairs), jnp.int32),
            pltpu.VMEM((1, NOCC), jnp.int32),
            pltpu.VMEM((1, window), jnp.int32),
            pltpu.VMEM((1, levels.shape[0]), jnp.float32),
            pltpu.VMEM((nz, owned, ndev, cols, qs), jnp.bfloat16),
            pltpu.VMEM((slabs, max(1, ny - 1), nz, owned, wide, qs), jnp.bfloat16),
            pltpu.VMEM((qs // LANES, window * (wide + 8), LANES), jnp.float32),
            pltpu.VMEM((cols * window, qs), jnp.bfloat16),
            pltpu.VMEM((cols // amp_c, pairs, amp_c, virt), jnp.bfloat16),
            pltpu.VMEM((virt // LANES, pairs * (amp_c + 8), LANES), jnp.float32),
            pltpu.VMEM((cols, pairs, virt), jnp.bfloat16),
            pltpu.VMEM((cols, nb * window, virt), jnp.bfloat16),
            pltpu.VMEM((nb * window, pairs), jnp.float32),
            pltpu.VMEM((nb, window, pairs), jnp.float32),
            pltpu.VMEM((nz, ndev, split, owned * pairs), jnp.float32),
            pltpu.VMEM((nba * nz, owned, owned * pairs), jnp.float32),
            pltpu.VMEM((nz * ndev, split, owned * pairs), jnp.float32),
            pltpu.VMEM((split // owned, nz * ndev, owned, owned * pairs), jnp.float32),
            dma,
            dma((4,)),
            dma((cols // amp_c,)),
            dma,
            dma,
            dma,
            dma,
            dma((2,)),
            dma((slabs, nz - 1)),
            dma((slabs, nz, max(1, no - 1))),
            dma((2,)),
            dma((slabs,)),
            dma((2,)),
        ],
        compiler_params=pltpu.CompilerParams(
            collective_id=0,
            has_side_effects=True,
            vmem_limit_bytes=(63 if nb * window > 512 else 56) << 20,
        ),
    )(
        factors,
        amplitudes,
        pair_order.reshape(1, -1),
        occ_bin.reshape(1, -1),
        vir_bin.reshape(1, -1),
        levels.reshape(1, -1),
    )


def solution(mesh):
    return jax.shard_map(
        functools.partial(per_device, mesh.shape["ba"], mesh.shape["dev"]),
        mesh=mesh,
        in_specs=(P("ba", "dev", None), P(None, "dev", None), P(), P(), P(), P()),
        out_specs=P("ba", "dev"),
        check_vma=False,
    )
```

```python
import functools

import jax
import jax.numpy as jnp
from jax import lax
from jax.experimental import pallas as pl
from jax.experimental.pallas import tpu as pltpu
from jax.sharding import PartitionSpec as P

NOCC = 8
LANES = 128
MESH = pl.DeviceIdType.MESH

level_shift = 0.3


def flip_bits(index, bits):
    result = index
    bit = 1
    while bit <= bits:
        if bits & bit:
            result = result + bit - 2 * bit * ((result // bit) % 2)
        bit *= 2
    return result


def to_column(row):
    n = row.shape[1]
    rows = lax.broadcasted_iota(jnp.int32, (n, n), 0)
    lanes = lax.broadcasted_iota(jnp.int32, (n, n), 1)
    return jnp.sum(jnp.where(rows == lanes, row, jnp.zeros_like(row)), axis=1, keepdims=True)


def kernel(
    dims,
    f_hbm,
    amps_hbm,
    order_hbm,
    occ_hbm,
    vir_hbm,
    levels_hbm,
    out_ref,
    order_ref,
    occ_ref,
    vir_ref,
    levels_ref,
    right,
    other,
    left_f32,
    left,
    raw,
    stage,
    amps,
    ints,
    flat,
    acc,
    tiles_s,
    tiles_f,
    parts_s,
    parts_f,
    own_sem,
    small_sem,
    amp_sem,
    sent_z,
    sent_x,
    sent_y,
    sent_c,
    sent_f,
    recv_z,
    recv_x,
    recv_c,
    recv_y,
    recv_f,
):
    nz, ny, no, owned, cols, qs, window, pairs, virt, amp_c, slabs = dims
    nd = no * 2
    nb = nz * owned
    total = nz * ny * nd
    split = window // nd
    wide = cols // slabs
    ba, dev = lax.axis_index("ba"), lax.axis_index("dev")
    me = ba * nd + dev
    z, y = ba // ny, ba % ny
    outer, core = dev // 2, dev % 2
    partner_core = outer * 2 + 1 - core
    chunks = cols // amp_c

    barrier = pltpu.get_barrier_semaphore()
    near = [(flip_bits(z, step) * ny + y, dev) for step in range(1, nz)]
    near += [(z * ny + flip_bits(y, step), dev) for step in range(1, ny)]
    near += [(ba, flip_bits(outer, step) * 2 + core) for step in range(1, no)]
    near.append((ba, partner_core))
    for there in near:
        pl.semaphore_signal(barrier, inc=1, device_id=there, device_id_type=MESH)

    def quarter(at_z):
        return pl.ds(pl.multiple_of(at_z * qs, LANES), qs)

    def factor_slab(slab, at_z):
        return f_hbm.at[:, pl.ds(slab * wide, wide), quarter(at_z)]

    own = pltpu.make_async_copy(f_hbm.at[:, :, quarter(z)], right.at[z, :, dev], own_sem)
    own.start()

    def amp_load(chunk):
        return pltpu.make_async_copy(
            amps_hbm.at[:, pl.ds(chunk * amp_c, amp_c), :], raw.at[chunk], amp_sem.at[chunk]
        )

    for chunk in range(chunks):
        amp_load(chunk).start()
    small = [
        pltpu.make_async_copy(source, target, small_sem.at[at])
        for at, (source, target) in enumerate(
            (
                (order_hbm, order_ref),
                (occ_hbm, occ_ref),
                (vir_hbm, vir_ref),
                (levels_hbm, levels_ref),
            )
        )
    ]
    for copy in small:
        copy.start()
    pl.semaphore_wait(barrier, len(near))

    def send(source, target, send_sem, recv_sem, ba_to, dev_to):
        copy = pltpu.make_async_remote_copy(
            src_ref=source,
            dst_ref=target,
            send_sem=send_sem,
            recv_sem=recv_sem,
            device_id=(ba_to, dev_to),
            device_id_type=MESH,
        )
        copy.start()

    def await_bytes(place, recv_sem):
        pltpu.make_async_remote_copy(
            src_ref=place,
            dst_ref=place,
            send_sem=sent_z,
            recv_sem=recv_sem,
            device_id=(ba, partner_core),
            device_id_type=MESH,
        ).wait_recv()

    def piece(slab, at_z, at_d):
        return right.at[at_z, :, at_d, pl.ds(slab * wide, wide), :]

    def to_partner(source, slab, step, at_d):
        at_z = flip_bits(z, step)
        send(source, piece(slab, at_z, at_d), sent_c, recv_c.at[min(step // 2, 1)], ba, partner_core)

    def source_of(slab, step):
        return piece(slab, flip_bits(z, step), dev) if step else factor_slab(slab, z)

    def spread_x(slab, step):
        source = source_of(slab, step)
        for other_outer in range(1, no):
            send(
                source,
                piece(slab, flip_bits(z, step), dev),
                sent_x,
                recv_x.at[slab, step, other_outer - 1],
                ba,
                flip_bits(outer, other_outer) * 2 + core,
            )
        to_partner(source, slab, step, dev)

    def spread_y(slab, step):
        for other_y in range(1, ny):
            send(
                source_of(slab, step),
                other.at[slab, other_y - 1, flip_bits(z, step)],
                sent_y,
                recv_y.at[slab],
                z * ny + flip_bits(y, other_y),
                dev,
            )

    def launch(slab, steps):
        for step in steps:
            at_z = flip_bits(z, step)
            send(
                factor_slab(slab, at_z),
                piece(slab, z, dev),
                sent_z,
                recv_z.at[slab, step - 1],
                at_z * ny + y,
                dev,
            )

    def land(slab, step):
        await_bytes(piece(slab, flip_bits(z, step), dev), recv_z.at[slab, step - 1])

    def from_z(slab, step):
        land(slab, step)
        spread_y(slab, step)
        spread_x(slab, step)

    def from_x(slab, step):
        for other_outer in range(1, no):
            at_d = flip_bits(outer, other_outer) * 2 + core
            place = piece(slab, flip_bits(z, step), at_d)
            await_bytes(place, recv_x.at[slab, step, other_outer - 1])
            to_partner(place, slab, step, at_d)

    def from_core(steps):
        await_bytes(right.at[0 : len(steps), :, 0:no], recv_c.at[min(steps[0] // 2, 1)])

    def widen(source, row):
        base = pl.multiple_of(row * (wide + 8), 8)
        for h in range(qs // LANES):
            left_f32[h, pl.ds(base, wide), :] = source[:, h * LANES : (h + 1) * LANES].astype(
                jnp.float32
            )

    def make_left(slab):
        if ny > 1:
            await_bytes(other.at[slab, 0 : ny - 1], recv_y.at[slab])
        for at_z in range(nz):
            for i in range(owned):
                widen(
                    right.at[at_z, i, dev, pl.ds(slab * wide, wide), :],
                    (at_z * ny + y) * owned + i,
                )
                for other_y in range(1, ny):
                    at_y = flip_bits(y, other_y)
                    widen(other.at[slab, other_y - 1, at_z, i], (at_z * ny + at_y) * owned + i)

        def turn(c, carry):
            rows = pl.ds(pl.multiple_of((slab * wide + c) * window, window), window)
            for h in range(qs // LANES):
                left[rows, h * LANES : (h + 1) * LANES] = left_f32[
                    h, pl.ds(c, window, stride=wide + 8), :
                ].astype(jnp.bfloat16)
            return carry

        lax.fori_loop(0, wide, turn, 0, unroll=wide)

    pitch = amp_c + 8

    def amp_chunk(chunk):
        amp_load(chunk).wait()
        for k in range(pairs):
            for h in range(virt // LANES):
                stage[h, k * pitch : k * pitch + amp_c, :] = raw[
                    chunk, k, :, h * LANES : (h + 1) * LANES
                ].astype(jnp.float32)
        for c in range(amp_c):
            for h in range(virt // LANES):
                amps[chunk * amp_c + c, :, h * LANES : (h + 1) * LANES] = stage[
                    h, pl.ds(c, pairs, stride=pitch), :
                ].astype(jnp.bfloat16)

    def integrals(first, count, steps):
        rows = left[first * wide * window : (first + count) * wide * window, :]
        for step in steps:
            for i in range(owned):
                side = right[flip_bits(z, step), i].reshape(virt, qs)
                at = (step * owned + i) * window
                ints[first * wide : (first + count) * wide, at : at + window, :] = (
                    lax.dot_general(
                        rows, side, (((1,), (1,)), ((), ())), preferred_element_type=jnp.float32
                    )
                    .astype(jnp.bfloat16)
                    .reshape(count * wide, window, virt)
                )

    def ladder(slab, steps):
        at, count = steps[0] * owned * window, len(steps) * owned * window
        span = range(slab * wide, (slab + 1) * wide)
        flat[at : at + count, :] += lax.dot_general(
            jnp.concatenate([ints[c, at : at + count, :] for c in span], axis=1),
            jnp.concatenate([amps[c] for c in span], axis=1),
            (((1,), (1,)), ((), ())),
            preferred_element_type=jnp.float32,
        )

    early, late = tuple(range(2)), tuple(range(2, nz))
    todo = list(range(chunks))

    def prepare(count=1):
        for chunk in todo[:count]:
            amp_chunk(chunk)
        del todo[:count]

    @pl.when(core == 1)
    def _():
        flat[0:8, :] = lax.fori_loop(
            0, 80, lambda at, value: value * 0.5 + 1.0, jnp.zeros((8, pairs), jnp.float32)
        )

    launch(0, (1,))
    for slab in range(1, min(2, slabs)):
        launch(slab, (1,))
    spread_x(0, 0)
    spread_y(0, 0)
    launch(0, late[:-1])
    prepare()
    for slab in range(2, slabs):
        launch(slab, (1,))
        if slab == 2:
            launch(0, late[-1:])
        spread_x(slab - 1, 0)
    if slabs < 3:
        launch(0, late[-1:])
    if slabs > 1:
        spread_x(slabs - 1, 0)
        spread_y(1, 0)
    prepare()
    for slab in range(1, slabs):
        launch(slab, late)
        prepare(slab % 2)
    flat[...] = jnp.zeros_like(flat)
    own.wait()
    from_z(0, 1)
    prepare()
    if slabs > 1:
        from_z(1, 1)
        prepare()
    from_x(0, 0)
    for step in late[:-1]:
        land(0, step)
        spread_y(0, step)
        prepare()
    for slab in range(2, slabs):
        land(slab, 1)
        spread_x(slab, 1)
        from_x(slab - 1, 0)
        prepare()
    land(0, nz - 1)
    spread_y(0, nz - 1)
    if slabs > 1:
        from_x(slabs - 1, 0)
    for step in late:
        spread_x(0, step)
    for slab in range(2, slabs):
        spread_y(slab, 0)
    prepare(chunks)
    for slab in range(slabs):
        from_x(slab, 1)

    def far_z(slab):
        if 0 < slab < slabs:
            for step in late:
                land(slab, step)
                spread_y(slab, step)
            for step in late:
                spread_x(slab, step)

    def far_x(slab):
        if slab < slabs:
            for step in late:
                from_x(slab, step)

    far_z(1)
    for slab in range(2, slabs):
        spread_y(slab, 1)
    for slab in range(slabs):
        make_left(slab)
        if slab == 0:
            from_core(early)
        integrals(slab, 1, early)
        if slab > 1:
            far_x(slab)
        far_z(slab + 2)
        ladder(slab, early)
        if slab < 2:
            far_x(slab)
    from_core(late)
    integrals(0, slabs, late)
    for slab in range(slabs):
        ladder(slab, late)

    for step in range(nz):
        for i in range(owned):
            at = (step * owned + i) * window
            acc[flip_bits(z, step) * owned + i] = flat[at : at + window, :]

    height = owned * split
    turns = split // owned
    here = z * nd + dev
    for at_z in range(nz):
        wide_row = jnp.concatenate([acc[at_z * owned + i] for i in range(owned)], axis=1)
        for at_d in range(nd):
            tiles_s[at_z, at_d] = wide_row[at_d * split : (at_d + 1) * split, :]
        for r in range(owned):
            turned = jnp.concatenate(
                [
                    acc[at_z * owned + r, pl.ds(i, window // owned, stride=owned), :]
                    for i in range(owned)
                ],
                axis=1,
            )
            for to_ba in range(window // owned):
                tiles_f[to_ba * nz + at_z, r : r + 1, :] = turned[to_ba : to_ba + 1, :]

    def post(source, target, at, to_ba, to_dev):
        there = to_ba * nd + to_dev

        @pl.when(there != me)
        def _():
            pltpu.make_async_remote_copy(
                src_ref=source,
                dst_ref=target,
                send_sem=sent_f.at[at],
                recv_sem=recv_f.at[at],
                device_id=(to_ba, to_dev),
                device_id_type=MESH,
            ).start()

        @pl.when(there == me)
        def _():
            pltpu.make_async_copy(source, target, recv_f.at[at]).start()

    def post_turned(to_ba, carry):
        for at_z in range(nz):
            owner = at_z * ny + y
            post(
                tiles_f.at[to_ba * nz + at_z],
                parts_f.at[owner % turns, here],
                1,
                to_ba,
                owner // turns,
            )
        return carry

    def post_straight(at_z, carry):
        for at_d in range(nd):
            post(tiles_s.at[at_z, at_d], parts_s.at[here], 0, at_z * ny + y, at_d)
        return carry

    if total <= 64:
        for to_ba in range(window // owned):
            if to_ba % ny == 0:
                post_straight(to_ba // ny, 0)
            post_turned(to_ba, 0)
    else:
        lax.fori_loop(0, nz, post_straight, 0)
        lax.fori_loop(0, window // owned, post_turned, 0)

    for copy in small:
        copy.wait()
    levels = to_column(levels_ref[...])
    level_at = lax.broadcasted_iota(jnp.int32, (levels.shape[0], window), 0)
    virtual = jnp.sum(
        jnp.where(level_at == vir_ref[...], levels, 0.0), axis=0, keepdims=True
    )
    level_occ = lax.broadcasted_iota(jnp.int32, (levels.shape[0], NOCC), 0)
    occupied = to_column(
        -jnp.sum(jnp.where(level_occ == occ_ref[...], levels, 0.0), axis=0, keepdims=True)
    )
    order = order_ref[...]
    first, second = order // NOCC, order % NOCC
    occ_at = lax.broadcasted_iota(jnp.int32, (NOCC, pairs), 0)
    pair_energy = jnp.sum(
        jnp.where(occ_at == first, occupied, 0.0), axis=0, keepdims=True
    ) + jnp.sum(jnp.where(occ_at == second, occupied, 0.0), axis=0, keepdims=True)
    win_row = lax.broadcasted_iota(jnp.int32, (height, window), 0)
    win_lane = lax.broadcasted_iota(jnp.int32, (height, window), 1)
    right_energy = jnp.sum(
        jnp.where(win_lane == ba * owned + win_row // split, virtual, 0.0), axis=1, keepdims=True
    )
    left_energy = jnp.sum(
        jnp.where(win_lane == dev * split + win_row % split, virtual, 0.0), axis=1, keepdims=True
    )
    denominator = right_energy + left_energy - pair_energy + level_shift
    permuter = (to_column(order) == second * NOCC + first).astype(jnp.float32)

    for at, place in enumerate((parts_s, parts_f)):
        pltpu.make_async_copy(place, place, recv_f.at[at]).wait()
    straight = jnp.sum(parts_s[...], axis=0)
    flipped = jnp.concatenate([jnp.sum(parts_f[j], axis=0) for j in range(turns)], axis=0)

    def stack(value):
        return jnp.concatenate(
            [value[:, i * pairs : (i + 1) * pairs] for i in range(owned)], axis=0
        )

    moved = jnp.dot(
        stack(flipped),
        permuter,
        precision=lax.Precision.HIGHEST,
        preferred_element_type=jnp.float32,
    )
    result = (stack(straight) + moved) / denominator
    for i in range(owned):
        for a in range(split):
            out_ref[i : i + 1, a * pairs : (a + 1) * pairs] = result[
                i * split + a : i * split + a + 1, :
            ]

    def await_sent(place, sem):
        pltpu.make_async_copy(place, place, sem).wait()

    await_sent(right.at[0 : nz - 1, :, 0], sent_z)
    await_sent(right.at[:, :, 0:no], sent_c)
    if no > 1:
        await_sent(right.at[:, :, 0 : no - 1], sent_x)
    if ny > 1:
        await_sent(other, sent_y)
    await_sent(parts_s.at[0 : nz * nd - 1], sent_f.at[0])
    kept = sum(
        jnp.where((at_z * ny + y) // turns == dev, 1, 0) for at_z in range(nz)
    )
    for count in range(2):

        @pl.when(kept == count)
        def _():
            await_sent(tiles_f.at[0 : tiles_f.shape[0] - count], sent_f.at[1])


def per_device(nba, ndev, factors, amplitudes, pair_order, occ_bin, vir_bin, levels):
    owned, cols, fitting = factors.shape
    pairs, _, virt = amplitudes.shape
    window = owned * nba
    ny = 1
    while ny * ny * 4 <= nba:
        ny *= 2
    nz = nba // ny
    no = ndev // 2
    qs = fitting // nz
    nb = nz * owned
    split = window // ndev
    amp_c = 16
    slabs = max(1, min(4, cols // 16))
    wide = cols // slabs
    dims = (nz, ny, no, owned, cols, qs, window, pairs, virt, amp_c, slabs)
    dma = pltpu.SemaphoreType.DMA
    vmem = pl.BlockSpec(memory_space=pltpu.VMEM)
    hbm = pl.BlockSpec(memory_space=pl.ANY)
    return pl.pallas_call(
        functools.partial(kernel, dims),
        out_shape=jax.ShapeDtypeStruct((owned, split * pairs), jnp.float32),
        in_specs=[hbm] * 6,
        out_specs=vmem,
        scratch_shapes=[
            pltpu.VMEM((1, pairs), jnp.int32),
            pltpu.VMEM((1, NOCC), jnp.int32),
            pltpu.VMEM((1, window), jnp.int32),
            pltpu.VMEM((1, levels.shape[0]), jnp.float32),
            pltpu.VMEM((nz, owned, ndev, cols, qs), jnp.bfloat16),
            pltpu.VMEM((slabs, max(1, ny - 1), nz, owned, wide, qs), jnp.bfloat16),
            pltpu.VMEM((qs // LANES, window * (wide + 8), LANES), jnp.float32),
            pltpu.VMEM((cols * window, qs), jnp.bfloat16),
            pltpu.VMEM((cols // amp_c, pairs, amp_c, virt), jnp.bfloat16),
            pltpu.VMEM((virt // LANES, pairs * (amp_c + 8), LANES), jnp.float32),
            pltpu.VMEM((cols, pairs, virt), jnp.bfloat16),
            pltpu.VMEM((cols, nb * window, virt), jnp.bfloat16),
            pltpu.VMEM((nb * window, pairs), jnp.float32),
            pltpu.VMEM((nb, window, pairs), jnp.float32),
            pltpu.VMEM((nz, ndev, split, owned * pairs), jnp.float32),
            pltpu.VMEM((nba * nz, owned, owned * pairs), jnp.float32),
            pltpu.VMEM((nz * ndev, split, owned * pairs), jnp.float32),
            pltpu.VMEM((split // owned, nz * ndev, owned, owned * pairs), jnp.float32),
            dma,
            dma((4,)),
            dma((cols // amp_c,)),
            dma,
            dma,
            dma,
            dma,
            dma((2,)),
            dma((slabs, nz - 1)),
            dma((slabs, nz, max(1, no - 1))),
            dma((2,)),
            dma((slabs,)),
            dma((2,)),
        ],
        compiler_params=pltpu.CompilerParams(
            collective_id=0,
            has_side_effects=True,
            vmem_limit_bytes=(63 if nb * window > 512 else 56) << 20,
        ),
    )(
        factors,
        amplitudes,
        pair_order.reshape(1, -1),
        occ_bin.reshape(1, -1),
        vir_bin.reshape(1, -1),
        levels.reshape(1, -1),
    )


def solution(mesh):
    return jax.shard_map(
        functools.partial(per_device, mesh.shape["ba"], mesh.shape["dev"]),
        mesh=mesh,
        in_specs=(P("ba", "dev", None), P(None, "dev", None), P(), P(), P(), P()),
        out_specs=P("ba", "dev"),
        check_vma=False,
    )
```
